32 devices in a mesh: slab: 4 (over y, core), bl: 8 (over z, x).
Axes of the slice: x: 2, y: 2, z: 4, core: 2. Of those that a mesh axis runs over, the one named last changes fastest.
Arguments:
- model_image: float32 [2, 8192, 8192], P(None, 'slab', 'bl'), may hold values from -6 to 6
- vis_coords: float32 [512, 2, 128], P(('slab', 'bl')), may hold values from 0 to 32
- vis_observed: float32 [512, 2, 128], P(('slab', 'bl')), may hold values from -6 to 6
- tile_slot: int32 [512], P(('slab', 'bl')), may hold values from 0 to 2047
- tile_group: int32 [512, 1], P(('slab', 'bl')), may hold values from 0 to 7; in each aligned block of 16 rows (0 to 15, 16 to 31, ...) at most 8 rows name the same one
- w_plane: int32 [512], P(('slab', 'bl')), may hold values from 0 to 7
- vis_count: int32 [512], P(('slab', 'bl')), may hold values from 16 to 128, as said below
Outputs:
- residual_image: float32 [2, 8192, 8192], P(None, 'slab', 'bl')
- residual_vis: float32 [512, 2, 128], P(('slab', 'bl'))
The draws below stay inside these ranges and needn't reach their ends.
Inputs may be any that keep to these rules, and one draw needn't show every extreme that they name: `tile_group`: among the 16 subgrids of one device, at most 8 name the same group. `vis_count`: some subgrid holds exactly 128 visibilities.
All inputs are finite; a program needn't handle non-finite values.
Results may differ from the reference program's by a relative error of at most 0.0003.
Values sent between devices are 32-bit elements; how exact they have to be, the bound alone decides.
A program may use at most 192 MiB of HBM per device.

```python
import math
import jax
import jax.numpy as jnp
import numpy as np
from jax import lax

N = 8192
SUB = 32
NW = 8
VPS = 128
SG_DEV = 16
CAP = 8
NSG = 512
NTILE = 256
TCOLS = 8
N_BL = 8


def draw_vis_count(key, part):
    counts = jax.random.randint(jax.random.fold_in(key, 11), (NSG,), VPS // 8, VPS + 1, dtype=jnp.int32)
    return counts.at[0].set(VPS)


def with_ends(array, rng, smallest, largest):
    spot = [jax.random.randint(jax.random.fold_in(rng, axis), (), 0, length) for axis, length in enumerate(array.shape)]
    widest = array.shape.index(max(array.shape))
    neighbour = spot[:widest] + [(spot[widest] + 1) % array.shape[widest]] + spot[widest + 1:]
    return array.at[tuple(spot)].set(smallest).at[tuple(neighbour)].set(largest)


def shard_levels(rng, extent, shards, smallest, top_value):
    level, own = 1.0, jax.random.fold_in(rng, 6)
    for axis_at, shards_of in shards:
        steps = jnp.exp(jax.random.uniform(jax.random.fold_in(own, axis_at), (shards_of,), jnp.float32, smallest / len(shards), top_value / len(shards)))
        level = level * jnp.repeat(steps, extent[axis_at] // shards_of).reshape([-1 if axis == axis_at else 1 for axis in range(len(extent))])
    return level


def assign_block(key, own, number, rows, amount, top, bound, lean):
    sequence = jax.random.permutation(key, amount)
    heavy_load, usual = shares(amount, rows * top, bound, lean, True), shares(amount, rows * top, bound, lean, False)
    places = jnp.arange(amount)

    def named(lengths, offset_by):
        used = int((lengths > 0).sum())
        fixed = max(1, used // 4)
        passed = fixed + (places - fixed + offset_by * (used - fixed)) % max(1, amount - fixed)
        return jnp.zeros((amount,), jnp.int32).at[sequence[jnp.where(places < fixed, places, passed)]].set(jnp.asarray(lengths, jnp.int32))

    lengths = jnp.where(number % 4 == 0, named(heavy_load, number // 4), named(usual, number - number // 4 - 1))
    mixed = jax.random.permutation(jax.random.fold_in(own, 3), amount)
    giver, receiver = mixed[0:amount // 2 * 2:2], mixed[1:amount // 2 * 2:2]
    margin = jnp.minimum(lengths[giver] - 1, bound - lengths[receiver]) // 2
    margin = jnp.where((giver == sequence[0]) | (receiver == sequence[0]) | (lengths[receiver] == 0), 0, jnp.maximum(margin, 0))
    passed = jax.random.randint(jax.random.fold_in(own, 4), (amount // 2,), 0, 1 << 20) % (margin + 1)
    lengths = lengths.at[giver].add(-passed).at[receiver].add(passed)
    labels = jnp.searchsorted(jnp.cumsum(lengths), jnp.arange(rows * top), side="right").astype(jnp.int32)
    table = labels.reshape(top, rows).T
    table = table[jax.random.permutation(jax.random.fold_in(own, 1), rows)]
    offset_by = jax.random.randint(jax.random.fold_in(own, 2), (rows, 1), 0, top)
    return jnp.take_along_axis(table, (jnp.arange(top)[None, :] + offset_by) % top, axis=1)


def shares(number_of, total, most, lean, full):
    weights = [(1 << 20) // math.isqrt(standing ** lean) + 1 for standing in range(1, number_of + 1)]
    largest = most if full else min(most, max(-(-total // number_of), total * weights[0] // sum(weights)))
    least = 1 if total - largest >= number_of - 1 else 0
    given, spare = [largest] + [least] * (number_of - 1), total - largest - least * (number_of - 1)
    while spare > 0:
        movable = [i for i in range(1, number_of) if given[i] < largest] or [i for i in range(1, number_of) if given[i] < most]
        pool, left = sum([weights[i] for i in movable]), spare
        for i in movable:
            addition = min(most - given[i], max(1, left * weights[i] // pool), spare)
            given[i] = given[i] + addition
            spare = spare - addition
    return np.array(given)


def normal_values(own_key, dims, deviation, reach, cuts=(), held_as=jnp.bfloat16):
    array = jax.random.normal(own_key, dims, jnp.float32) * deviation
    if len(cuts) > 0:
        array = shard_levels(own_key, dims, cuts, -0.22, 0.18) * array
    return jnp.clip(array, min=-reach, max=reach).astype(held_as)


def setup_inputs(seed: int = 0) -> dict:
    seeds = jax.random.split(jax.random.key(seed), 8)
    model_image = normal_values(seeds[0], (2, N, N), 1.0, 6.0, ((1, 4), (2, 8)), jnp.float32)
    vis_coords = jnp.clip(32.0 * jax.random.uniform(seeds[1], (NSG, 2, VPS), jnp.float32) ** shard_levels(seeds[1], (NSG, 2, VPS), ((0, 32),), -0.2, 0.2), 0.0, 32.0)
    vis_observed = normal_values(seeds[2], (NSG, 2, VPS), 1.0, 6.0, ((0, 32),), jnp.float32)
    tile_slot = with_ends(jax.random.randint(seeds[3], (NSG,), 0, NTILE * TCOLS), jax.random.fold_in(seeds[3], 1), 0, (NTILE * TCOLS) - 1).astype(jnp.int32)
    tile_group_keys = jax.random.split(jax.random.fold_in(seeds[4], 1), NSG // SG_DEV)
    tile_group_turns = jax.random.permutation(jax.random.fold_in(seeds[4], 3), NSG // SG_DEV)
    tile_group = jax.vmap(lambda own, number: assign_block(jax.random.fold_in(seeds[4], 2), own, number, SG_DEV, N_BL, 1, CAP, 2))(tile_group_keys, tile_group_turns).reshape((NSG, 1))
    w_plane = with_ends(jax.random.randint(seeds[5], (NSG,), 0, NW), jax.random.fold_in(seeds[5], 1), 0, NW - 1).astype(jnp.int32)
    vis_count = draw_vis_count(jax.random.fold_in(seeds[7], 71), 0)
    return {"model_image": model_image, "vis_coords": vis_coords, "vis_observed": vis_observed, "tile_slot": tile_slot, "tile_group": tile_group, "w_plane": w_plane, "vis_count": vis_count}


w_step = 0.1


def complex_einsum(form, left, right):
    product = lambda first, second: jnp.einsum(form, first, second, precision=lax.Precision.HIGHEST)
    return (product(left[0], right[0]) - product(left[1], right[1]),
            product(left[0], right[1]) + product(left[1], right[0]))


def complex_mul(left, right):
    return (left[0] * right[0] - left[1] * right[1], left[0] * right[1] + left[1] * right[0])


def subgrid_pass(tile_real, tile_imag, coords, observed, planes, counts):
    width = tile_real.shape[-1]
    half = width // 2
    slots = coords.shape[-1]
    index = jnp.arange(width, dtype=jnp.int32)
    offsets = (index - half).astype(jnp.float32)
    turns = (index[:, None] * (index[None, :] - half)) % width
    angle = (2.0 * math.pi / width) * turns.astype(jnp.float32)
    forward_d = (jnp.cos(angle), jnp.sin(angle))
    backward_d = (forward_d[0], -forward_d[1])
    scale_sub = 1.0 / (width * width)
    halfway = complex_einsum('il,kij->klj', forward_d, (tile_real, tile_imag))
    image_sub = complex_einsum('klj,jm->klm', halfway, forward_d)
    image_sub = (image_sub[0] * scale_sub, image_sub[1] * scale_sub)
    radius = (offsets[:, None] ** 2 + offsets[None, :] ** 2) / (half * half)
    phase = -w_step * planes.astype(jnp.float32)[:, None, None] * radius[None]
    screen = (jnp.cos(phase), jnp.sin(phase))
    weighted = complex_mul(screen, image_sub)
    along_a = (-2.0 * math.pi / width) * coords[:, 0, :][:, None, :] * offsets[None, :, None]
    along_b = (-2.0 * math.pi / width) * coords[:, 1, :][:, None, :] * offsets[None, :, None]
    phase_a = (jnp.cos(along_a), jnp.sin(along_a))
    phase_b = (jnp.cos(along_b), jnp.sin(along_b))
    partial_rows = complex_einsum('klm,kmj->klj', weighted, phase_b)
    terms = complex_mul(phase_a, partial_rows)
    predicted = (jnp.sum(terms[0], axis=1), jnp.sum(terms[1], axis=1))
    live = (jnp.arange(slots, dtype=jnp.int32)[None, :] < counts[:, None]).astype(jnp.float32)
    resid_real = (observed[:, 0, :] - predicted[0]) * live
    resid_imag = (observed[:, 1, :] - predicted[1]) * live
    spread = complex_mul((phase_a[0], -phase_a[1]), (resid_real[:, None, :], resid_imag[:, None, :]))
    collected = complex_einsum('klj,kmj->klm', spread, (phase_b[0], -phase_b[1]))
    unscreened = complex_mul((screen[0], -screen[1]), collected)
    middle = complex_einsum('il,klm->kim', backward_d, unscreened)
    tile_out = complex_einsum('kim,jm->kij', middle, backward_d)
    return (jnp.stack([resid_real, resid_imag], axis=1),
            jnp.stack([tile_out[0] * scale_sub, tile_out[1] * scale_sub], axis=1))


def reference(model_image, vis_coords, vis_observed, tile_slot, tile_group, w_plane, vis_count):
    image = lax.complex(model_image[0], model_image[1])
    grid = jnp.fft.fft2(image) / N
    tiles = grid.reshape(NTILE, SUB, NTILE, SUB).transpose(0, 2, 1, 3).reshape(NTILE * NTILE, SUB, SUB)
    index = jnp.arange(NSG, dtype=jnp.int32)
    band = index // (SG_DEV * N_BL)
    column = (band * N_BL + tile_group[:, 0]) * TCOLS + tile_slot // NTILE
    tile_id = ((tile_slot % NTILE) * NTILE + column).astype(jnp.int32)
    blocks = NSG // SG_DEV

    def one_block(pieces):
        block_ids, block_coords, block_obs, block_planes, block_counts = pieces
        chosen = tiles[block_ids]
        return subgrid_pass(jnp.real(chosen), jnp.imag(chosen), block_coords, block_obs, block_planes, block_counts)

    resid_vis, contrib = lax.map(one_block, (
        tile_id.reshape(blocks, SG_DEV),
        vis_coords.reshape(blocks, SG_DEV, 2, VPS),
        vis_observed.reshape(blocks, SG_DEV, 2, VPS),
        w_plane.reshape(blocks, SG_DEV),
        vis_count.reshape(blocks, SG_DEV)))
    resid_vis = resid_vis.reshape(NSG, 2, VPS)
    contrib = contrib.reshape(NSG, 2 * SUB * SUB)
    summed = jax.ops.segment_sum(contrib, tile_id, num_segments=NTILE * NTILE)
    resid_grid = summed.reshape(NTILE, NTILE, 2, SUB, SUB).transpose(2, 0, 3, 1, 4).reshape(2, N, N)
    back = jnp.fft.ifft2(lax.complex(resid_grid[0], resid_grid[1])) * N
    resid_image = jnp.stack([jnp.real(back), jnp.imag(back)]).astype(jnp.float32)
    return resid_image, resid_vis
```

```python
import functools
import math

import jax
import jax.numpy as jnp
import numpy as np
from jax import lax
from jax.experimental import pallas as pl
from jax.experimental.pallas import tpu as pltpu
from jax.sharding import PartitionSpec as P

SUB = 32
LANES = 128
F32, BF16 = jnp.float32, jnp.bfloat16

w_step = 0.1


def complex_einsum(form, left, right):
    product = lambda first, second: jnp.einsum(form, first, second, precision=lax.Precision.HIGHEST)
    return (
        product(left[0], right[0]) - product(left[1], right[1]),
        product(left[0], right[1]) + product(left[1], right[0]),
    )


def complex_mul(left, right):
    return (left[0] * right[0] - left[1] * right[1], left[0] * right[1] + left[1] * right[0])


def subgrid_pass(tile_real, tile_imag, coords, observed, planes, counts):
    width = tile_real.shape[-1]
    half = width // 2
    slots = coords.shape[-1]
    index = jnp.arange(width, dtype=jnp.int32)
    offsets = (index - half).astype(jnp.float32)
    turns = index[:, None] * (index[None, :] - half) % width
    angle = 2.0 * math.pi / width * turns.astype(jnp.float32)
    forward_d = (jnp.cos(angle), jnp.sin(angle))
    backward_d = (forward_d[0], -forward_d[1])
    scale_sub = 1.0 / (width * width)
    halfway = complex_einsum("il,kij->klj", forward_d, (tile_real, tile_imag))
    image_sub = complex_einsum("klj,jm->klm", halfway, forward_d)
    image_sub = (image_sub[0] * scale_sub, image_sub[1] * scale_sub)
    radius = (offsets[:, None] ** 2 + offsets[None, :] ** 2) / (half * half)
    phase = -w_step * planes.astype(jnp.float32)[:, None, None] * radius[None]
    screen = (jnp.cos(phase), jnp.sin(phase))
    weighted = complex_mul(screen, image_sub)
    along_a = -2.0 * math.pi / width * coords[:, 0, :][:, None, :] * offsets[None, :, None]
    along_b = -2.0 * math.pi / width * coords[:, 1, :][:, None, :] * offsets[None, :, None]
    phase_a = (jnp.cos(along_a), jnp.sin(along_a))
    phase_b = (jnp.cos(along_b), jnp.sin(along_b))
    partial_rows = complex_einsum("klm,kmj->klj", weighted, phase_b)
    terms = complex_mul(phase_a, partial_rows)
    predicted = (jnp.sum(terms[0], axis=1), jnp.sum(terms[1], axis=1))
    live = (jnp.arange(slots, dtype=jnp.int32)[None, :] < counts[:, None]).astype(jnp.float32)
    resid_real = (observed[:, 0, :] - predicted[0]) * live
    resid_imag = (observed[:, 1, :] - predicted[1]) * live
    spread = complex_mul(
        (phase_a[0], -phase_a[1]), (resid_real[:, None, :], resid_imag[:, None, :])
    )
    collected = complex_einsum("klj,kmj->klm", spread, (phase_b[0], -phase_b[1]))
    unscreened = complex_mul((screen[0], -screen[1]), collected)
    middle = complex_einsum("il,klm->kim", backward_d, unscreened)
    tile_out = complex_einsum("kim,jm->kij", middle, backward_d)
    return (
        jnp.stack([resid_real, resid_imag], axis=1),
        jnp.stack([tile_out[0] * scale_sub, tile_out[1] * scale_sub], axis=1),
    )


def turn(value, modulus):
    angle = 2.0 * math.pi / modulus * (value % modulus).astype(F32)
    return jnp.cos(angle), jnp.sin(angle)


def split(value):
    high = lax.reduce_precision(value, 8, 7)
    return high.astype(BF16), (value - high).astype(BF16)


def split_in(value):
    high = value.astype(BF16)
    return high, (value - high.astype(F32)).astype(BF16)


def times_unit(pair, numerator, denominator):
    re, im = pair
    eighth = 8 * numerator % (8 * denominator)
    if eighth % denominator == 0:
        eighth //= denominator
        r = math.sqrt(0.5)
        if eighth == 0:
            return re, im
        if eighth == 2:
            return -im, re
        if eighth == 4:
            return -re, -im
        if eighth == 6:
            return im, -re
        if eighth == 1:
            return (re - im) * r, (re + im) * r
        if eighth == 3:
            return (re + im) * -r, (re - im) * r
        if eighth == 5:
            return (im - re) * r, (re + im) * -r
        return (re + im) * r, (im - re) * r
    angle = 2.0 * math.pi * (numerator % denominator) / denominator
    c, s = math.cos(angle), math.sin(angle)
    return re * c - im * s, re * s + im * c


def small_fft(values, sign):
    n = len(values)
    if n == 1:
        return values
    even, odd = small_fft(values[0::2], sign), small_fft(values[1::2], sign)
    out = [None] * n
    for k in range(n // 2):
        re, im = times_unit(odd[k], sign * k, n)
        out[k] = (even[k][0] + re, even[k][1] + im)
        out[k + n // 2] = (even[k][0] - re, even[k][1] - im)
    return out


def forward_kernel(
    tu_ref, image_ref, other_ref, dft2_ref, dft1_ref, turn_ref, col_ref, e_ref, out_ref,
    x_buf, z_buf, u_buf, lhs_buf, sems, *, ntile, blocks, chunk,
):
    step = pl.program_id(0)
    core = lax.rem(lax.axis_index("slab"), 2)
    kr = x_buf.shape[2]
    half = kr // 2
    per = SUB // kr
    tiles = ntile // 16

    def copies(block, slot):
        mine = pl.multiple_of(core * (blocks * LANES) + block * LANES, LANES)
        theirs = pl.multiple_of(block * LANES, LANES)
        return (
            pltpu.make_async_copy(
                image_ref.at[:, :, :, pl.ds(mine, LANES)],
                x_buf.at[slot, :, pl.ds(core * half, half)], sems.at[slot, 0]),
            pltpu.make_async_copy(
                other_ref.at[:, :, :, pl.ds(theirs, LANES)],
                x_buf.at[slot, :, pl.ds((1 - core) * half, half)], sems.at[slot, 1]),
        )

    @pl.when(step == 0)
    def _():
        for copy in copies(0, 0):
            copy.start()

        def one_block(block, carry):
            slot = lax.rem(block, 2)

            @pl.when(block + 1 < blocks)
            def _():
                for copy in copies(block + 1, 1 - slot):
                    copy.start()

            for copy in copies(block, slot):
                copy.wait()

            def rows(tile, carry):
                at = pl.ds(pl.multiple_of(tile * 16, 16), 16)
                turns = turn_ref[at, :]
                for q in range(per):
                    values = []
                    for k in range(kr):
                        pair = (x_buf[slot, 0, k, at, :], x_buf[slot, 1, k, at, :])
                        values.append(times_unit(pair, -q * k, SUB))
                    for m, (re, im) in enumerate(small_fft(values, -1)):
                        i = per * m + q
                        c = jnp.broadcast_to(turns[:, 2 * i:2 * i + 1], re.shape)
                        s = jnp.broadcast_to(turns[:, 2 * i + 1:2 * i + 2], re.shape)
                        lane = pl.ds(i % 2 * LANES, LANES)
                        for part, value in enumerate((re * c + im * s, im * c - re * s)):
                            high, low = split_in(value)
                            z_buf[i // 2, part, at, lane] = high
                            z_buf[i // 2, part + 2, at, lane] = low
                return carry

            lax.fori_loop(0, tiles, rows, 0)

            def pairs(pair, carry):
                z = z_buf[pair].reshape(4 * ntile, 2 * LANES)
                u = jnp.dot(dft2_ref[...], z, preferred_element_type=F32)
                u += jnp.dot(dft1_ref[...], z[:2 * ntile], preferred_element_type=F32)
                for part in range(2):
                    for side in range(2):
                        plane = pl.multiple_of((part * SUB + pair * 2 + side) * ntile, ntile)
                        u_buf[block, pl.ds(plane, ntile), :] = u[
                            part * ntile:(part + 1) * ntile, side * LANES:(side + 1) * LANES]
                return carry

            lax.fori_loop(0, SUB // 2, pairs, 0)
            return carry

        lax.fori_loop(0, blocks, one_block, 0)

    wide = blocks * LANES

    def one(g, carry):
        tu = tu_ref[step * chunk + g]
        rows = pl.ds(pl.multiple_of(g * SUB, SUB), SUB)
        for block in range(blocks):
            x = u_buf[block, pl.ds(tu, 2 * SUB, ntile), :]
            c, s = e_ref[g, 2 * block:2 * block + 1, :], e_ref[g, 2 * block + 1:2 * block + 2, :]
            re, im = x[:SUB], x[SUB:]
            for part, value in enumerate((re * c + im * s, im * c - re * s)):
                high, low = split_in(value)
                lhs_buf[rows, pl.ds(part * wide + block * LANES, LANES)] = high
                lhs_buf[rows, pl.ds((part + 2) * wide + block * LANES, LANES)] = low
        return carry

    lax.fori_loop(0, chunk, one, 0, unroll=2)
    made = jnp.dot(lhs_buf[...], col_ref[...], preferred_element_type=F32)
    made = made + pltpu.roll(made, LANES // 2, 1)
    made = made.reshape(chunk, SUB, LANES)
    left = lax.broadcasted_iota(jnp.int32, (chunk, SUB // 2, LANES), 2) < LANES // 2
    out_ref[...] = jnp.where(left, made[:, :SUB // 2], made[:, SUB // 2:])


def backward_kernel(
    tu_ref, c_ref, dft2_ref, dft1_ref, turn_ref, col_ref, e_ref, image_ref, other_ref,
    x_buf, y_buf, s_buf, p_buf, sems, *, ntile, blocks, chunk, steps,
):
    step = pl.program_id(0)
    core = lax.rem(lax.axis_index("slab"), 2)
    kr = x_buf.shape[2]
    half = kr // 2
    per = SUB // kr
    wide = blocks * LANES

    @pl.when(step == 0)
    def _():
        zero = jnp.zeros((ntile, LANES), F32)

        def clear(plane, carry):
            for block in range(blocks):
                s_buf[block, pl.ds(pl.multiple_of(plane * ntile, ntile), ntile), :] = zero
            return carry

        lax.fori_loop(0, 2 * SUB, clear, 0)

    given = c_ref[...]
    turned = pltpu.roll(given.reshape(chunk * SUB // 2, LANES), LANES // 2, 1).reshape(given.shape)
    left = lax.broadcasted_iota(jnp.int32, given.shape, 2) < LANES // 2
    both = jnp.concatenate([jnp.where(left, given, turned), jnp.where(left, turned, given)], axis=1)
    high, low = split_in(both.reshape(chunk * SUB, LANES))
    p_buf[...] = jnp.dot(jnp.concatenate([high, low], axis=1), col_ref[...], preferred_element_type=F32)

    def one(g, carry):
        tu = tu_ref[step * chunk + g]
        rows = pl.ds(pl.multiple_of(g * SUB, SUB), SUB)
        for block in range(blocks):
            re = p_buf[rows, pl.ds(block * LANES, LANES)]
            im = p_buf[rows, pl.ds(wide + block * LANES, LANES)]
            c, s = e_ref[g, 2 * block:2 * block + 1, :], e_ref[g, 2 * block + 1:2 * block + 2, :]
            at = pl.ds(tu, 2 * SUB, ntile)
            s_buf[block, at, :] = s_buf[block, at, :] + jnp.concatenate(
                [re * c - im * s, re * s + im * c], axis=0)
        return carry

    lax.fori_loop(0, chunk, one, 0, unroll=2)

    def copies(block, slot):
        mine = pl.multiple_of(core * wide + block * LANES, LANES)
        theirs = pl.multiple_of(block * LANES, LANES)
        return (
            pltpu.make_async_copy(
                x_buf.at[slot, :, pl.ds(core * half, half)],
                image_ref.at[:, :, :, pl.ds(mine, LANES)], sems.at[slot, 0]),
            pltpu.make_async_copy(
                x_buf.at[slot, :, pl.ds((1 - core) * half, half)],
                other_ref.at[:, :, :, pl.ds(theirs, LANES)], sems.at[slot, 1]),
        )

    @pl.when(step == steps - 1)
    def _():
        def one_block(block, carry):
            slot = lax.rem(block, 2)

            def pairs(pair, carry):
                parts = []
                for part in range(2):
                    sides = []
                    for side in range(2):
                        plane = pl.multiple_of((part * SUB + pair * 2 + side) * ntile, ntile)
                        sides.append(s_buf[block, pl.ds(plane, ntile), :])
                    parts.append(jnp.concatenate(sides, axis=1))
                high, low = split_in(jnp.concatenate(parts, axis=0))
                y = jnp.dot(dft2_ref[...], jnp.concatenate([high, low], axis=0), preferred_element_type=F32)
                y += jnp.dot(dft1_ref[...], high, preferred_element_type=F32)
                for part in range(2):
                    for side in range(2):
                        y_buf[pair * 2 + side, part] = y[
                            part * ntile:(part + 1) * ntile, side * LANES:(side + 1) * LANES]
                return carry

            lax.fori_loop(0, SUB // 2, pairs, 0)

            @pl.when(block >= 2)
            def _():
                for copy in copies(block - 2, slot):
                    copy.wait()

            def rows(tile, carry):
                at = pl.ds(pl.multiple_of(tile * 8, 8), 8)
                turns = turn_ref[at, :]
                total = [None] * kr
                for q in range(per):
                    values = []
                    for m in range(kr):
                        i = per * m + q
                        re, im = y_buf[i, 0, at, :], y_buf[i, 1, at, :]
                        c = jnp.broadcast_to(turns[:, 2 * i:2 * i + 1], re.shape)
                        s = jnp.broadcast_to(turns[:, 2 * i + 1:2 * i + 2], re.shape)
                        values.append((re * c - im * s, re * s + im * c))
                    for k, value in enumerate(small_fft(values, 1)):
                        re, im = times_unit(value, q * k, SUB)
                        total[k] = (re, im) if q == 0 else (total[k][0] + re, total[k][1] + im)
                for k in range(kr):
                    x_buf[slot, 0, k, at, :] = total[k][0]
                    x_buf[slot, 1, k, at, :] = total[k][1]
                return carry

            lax.fori_loop(0, ntile // 8, rows, 0)
            for copy in copies(block, slot):
                copy.start()
            return carry

        lax.fori_loop(0, blocks, one_block, 0)
        for block in range(max(0, blocks - 2), blocks):
            for copy in copies(block, block % 2):
                copy.wait()


def complex_table(cos, sin):
    return jnp.concatenate(
        [jnp.concatenate([cos, -sin], axis=1), jnp.concatenate([sin, cos], axis=1)], axis=0)


def per_device(model_image, vis_coords, vis_observed, tile_slot, tile_group, w_plane, vis_count):
    groups = lax.axis_size("bl")
    bands = lax.axis_size("slab")
    both = ("slab", "bl")
    rows, cols = model_image.shape[1:]
    length = rows * bands
    ntile = length // SUB
    band = lax.axis_index("slab")
    core = lax.rem(band, 2)
    wide = cols // 2
    blocks = wide // LANES
    kr = 2 * rows // ntile
    swap = [(d, d ^ 1) for d in range(bands)]

    leaving = lax.dynamic_slice_in_dim(model_image, (1 - core) * wide, wide, axis=2)
    other = lax.ppermute(leaving, "slab", swap)

    sub_count = tile_slot.shape[0]
    tile_cols = ntile // (bands * groups)
    own_tv = (band * groups + tile_group[:, 0]) * tile_cols + tile_slot // ntile
    own_tu = tile_slot % ntile
    named = lax.all_gather(jnp.stack([own_tu, own_tv], axis=0), both, axis=1, tiled=True)
    tu, tv = named[0], named[1]
    total = tu.shape[0]
    chunk = math.gcd(total, 16)
    steps = total // chunk

    inner = jnp.arange(ntile, dtype=jnp.int32)
    outer = jnp.arange(SUB, dtype=jnp.int32)
    own_cols = lax.axis_index("bl") * cols + core * wide + jnp.arange(wide, dtype=jnp.int32)
    first_row = band // 2 * (2 * rows)

    dft_c, dft_s = turn(inner[:, None] * inner[None, :], ntile)
    fwd_high, fwd_low = split(complex_table(dft_c, -dft_s))
    bwd_high, bwd_low = split(complex_table(dft_c, dft_s))
    turns = jnp.stack(turn((first_row + inner)[:, None] * outer[None, :], length), axis=2)
    turns = jnp.pad(turns.reshape(ntile, 2 * SUB), ((0, 0), (0, LANES - 2 * SUB)))
    col_c, col_s = turn(own_cols[:, None] * outer[None, :], length)
    col_c, col_s = col_c / length, col_s / length
    out_high, out_low = split(jnp.concatenate(
        [jnp.concatenate([col_c, -col_s], axis=1), jnp.concatenate([col_s, col_c], axis=1)], axis=0))
    zero = jnp.zeros_like(out_high)
    col_fwd = jnp.concatenate(
        [jnp.concatenate([out_high, out_low], axis=1), jnp.concatenate([out_high, zero], axis=1)], axis=0)
    in_high, in_low = split(jnp.concatenate(
        [jnp.concatenate([col_c.T, col_s.T], axis=1), jnp.concatenate([-col_s.T, col_c.T], axis=1)], axis=0))
    col_bwd = jnp.concatenate([in_high, in_low, in_high, in_low], axis=0)
    e_c, e_s = turn(tv[:, None] * own_cols[None, :], ntile)
    e_table = jnp.stack([e_c.reshape(total, blocks, LANES), e_s.reshape(total, blocks, LANES)], axis=2)
    e_table = e_table.reshape(total, 2 * blocks, LANES)

    whole = lambda shape: pl.BlockSpec(shape, lambda step, ids: (0,) * len(shape))
    by_step = lambda shape: pl.BlockSpec(shape, lambda step, ids: (step,) + (0,) * (len(shape) - 1))
    anywhere = pl.BlockSpec(memory_space=pl.ANY)
    params = pltpu.CompilerParams(
        dimension_semantics=("arbitrary",), vmem_limit_bytes=67_000_000)
    partial = pl.pallas_call(
        functools.partial(forward_kernel, ntile=ntile, blocks=blocks, chunk=chunk),
        grid_spec=pltpu.PrefetchScalarGridSpec(
            num_scalar_prefetch=1,
            grid=(steps,),
            in_specs=[
                anywhere, anywhere,
                whole((2 * ntile, 4 * ntile)), whole((2 * ntile, 2 * ntile)), whole((ntile, LANES)),
                whole((4 * wide, LANES)), by_step((chunk, 2 * blocks, LANES)),
            ],
            out_specs=by_step((chunk, SUB // 2, LANES)),
            scratch_shapes=[
                pltpu.VMEM((2, 2, kr, ntile, LANES), F32),
                pltpu.VMEM((SUB // 2, 4, ntile, 2 * LANES), BF16),
                pltpu.VMEM((blocks, 2 * SUB * ntile, LANES), F32),
                pltpu.VMEM((chunk * SUB, 4 * wide), BF16),
                pltpu.SemaphoreType.DMA((2, 2)),
            ],
        ),
        out_shape=jax.ShapeDtypeStruct((total, SUB // 2, LANES), F32),
        compiler_params=params,
        name="tiles_from_image",
    )(
        tu,
        model_image.reshape(2, kr // 2, ntile, cols), other.reshape(2, kr // 2, ntile, wide),
        jnp.concatenate([fwd_high, fwd_high], axis=1), fwd_low, turns, col_fwd, e_table,
    )
    mine = lax.psum_scatter(partial, both, scatter_dimension=0, tiled=True)
    mine = mine.reshape(sub_count, SUB // 2, 2, 2, SUB).transpose(3, 0, 2, 1, 4)
    mine = mine.reshape(2, sub_count, SUB, SUB)
    residual_vis, contrib = subgrid_pass(
        mine[0], mine[1], vis_coords, vis_observed, w_plane, vis_count)
    contrib = contrib.reshape(sub_count, 2, 2, SUB // 2, SUB).transpose(0, 3, 2, 1, 4)
    everyone = lax.all_gather(contrib.reshape(sub_count, SUB // 2, LANES), both, tiled=True)

    image, leaving = pl.pallas_call(
        functools.partial(backward_kernel, ntile=ntile, blocks=blocks, chunk=chunk, steps=steps),
        grid_spec=pltpu.PrefetchScalarGridSpec(
            num_scalar_prefetch=1,
            grid=(steps,),
            in_specs=[
                by_step((chunk, SUB // 2, LANES)),
                whole((2 * ntile, 4 * ntile)), whole((2 * ntile, 2 * ntile)), whole((ntile, LANES)),
                whole((8 * SUB, 2 * wide)), by_step((chunk, 2 * blocks, LANES)),
            ],
            out_specs=[anywhere, anywhere],
            scratch_shapes=[
                pltpu.VMEM((2, 2, kr, ntile, LANES), F32),
                pltpu.VMEM((SUB, 2, ntile, LANES), F32),
                pltpu.VMEM((blocks, 2 * SUB * ntile, LANES), F32),
                pltpu.VMEM((chunk * SUB, 2 * wide), F32),
                pltpu.SemaphoreType.DMA((2, 2)),
            ],
        ),
        out_shape=[
            jax.ShapeDtypeStruct((2, kr // 2, ntile, cols), F32),
            jax.ShapeDtypeStruct((2, kr // 2, ntile, wide), F32),
        ],
        compiler_params=params,
        name="image_from_tiles",
    )(
        tu, everyone,
        jnp.concatenate([bwd_high, bwd_high], axis=1), bwd_low, turns, col_bwd, e_table,
    )
    arrived = lax.ppermute(leaving.reshape(2, rows, wide), "slab", swap)
    image = lax.dynamic_update_slice_in_dim(
        image.reshape(2, rows, cols), arrived, (1 - core) * wide, axis=2)
    return (image, residual_vis)


def solution(mesh):
    placed = (
        P(None, "slab", "bl"),
        P(("slab", "bl"), None, None),
        P(("slab", "bl"), None, None),
        P(("slab", "bl")),
        P(("slab", "bl"), None),
        P(("slab", "bl")),
        P(("slab", "bl")),
    )
    return jax.shard_map(
        per_device,
        mesh=mesh,
        in_specs=placed,
        out_specs=(P(None, "slab", "bl"), P(("slab", "bl"), None, None)),
        check_vma=False,
    )
```

```python
import functools
import math

import jax
import jax.numpy as jnp
import numpy as np
from jax import lax
from jax.experimental import pallas as pl
from jax.experimental.pallas import tpu as pltpu
from jax.sharding import PartitionSpec as P

SUB = 32
LANES = 128
F32, BF16 = jnp.float32, jnp.bfloat16

w_step = 0.1


def complex_einsum(form, left, right):
    product = lambda first, second: jnp.einsum(form, first, second, precision=lax.Precision.HIGH)
    return (
        product(left[0], right[0]) - product(left[1], right[1]),
        product(left[0], right[1]) + product(left[1], right[0]),
    )


def complex_mul(left, right):
    return (left[0] * right[0] - left[1] * right[1], left[0] * right[1] + left[1] * right[0])


def subgrid_pass(tile_real, tile_imag, coords, observed, planes, counts):
    width = tile_real.shape[-1]
    half = width // 2
    slots = coords.shape[-1]
    index = jnp.arange(width, dtype=jnp.int32)
    offsets = (index - half).astype(jnp.float32)
    turns = index[:, None] * (index[None, :] - half) % width
    angle = 2.0 * math.pi / width * turns.astype(jnp.float32)
    forward_d = (jnp.cos(angle), jnp.sin(angle))
    backward_d = (forward_d[0], -forward_d[1])
    scale_sub = 1.0 / (width * width)
    halfway = complex_einsum("il,kij->klj", forward_d, (tile_real, tile_imag))
    image_sub = complex_einsum("klj,jm->klm", halfway, forward_d)
    image_sub = (image_sub[0] * scale_sub, image_sub[1] * scale_sub)
    radius = (offsets[:, None] ** 2 + offsets[None, :] ** 2) / (half * half)
    phase = -w_step * planes.astype(jnp.float32)[:, None, None] * radius[None]
    screen = (jnp.cos(phase), jnp.sin(phase))
    weighted = complex_mul(screen, image_sub)
    along_a = -2.0 * math.pi / width * coords[:, 0, :][:, None, :] * offsets[None, :, None]
    along_b = -2.0 * math.pi / width * coords[:, 1, :][:, None, :] * offsets[None, :, None]
    phase_a = (jnp.cos(along_a), jnp.sin(along_a))
    phase_b = (jnp.cos(along_b), jnp.sin(along_b))
    partial_rows = complex_einsum("klm,kmj->klj", weighted, phase_b)
    terms = complex_mul(phase_a, partial_rows)
    predicted = (jnp.sum(terms[0], axis=1), jnp.sum(terms[1], axis=1))
    live = (jnp.arange(slots, dtype=jnp.int32)[None, :] < counts[:, None]).astype(jnp.float32)
    resid_real = (observed[:, 0, :] - predicted[0]) * live
    resid_imag = (observed[:, 1, :] - predicted[1]) * live
    spread = complex_mul(
        (phase_a[0], -phase_a[1]), (resid_real[:, None, :], resid_imag[:, None, :])
    )
    collected = complex_einsum("klj,kmj->klm", spread, (phase_b[0], -phase_b[1]))
    unscreened = complex_mul((screen[0], -screen[1]), collected)
    middle = complex_einsum("il,klm->kim", backward_d, unscreened)
    tile_out = complex_einsum("kim,jm->kij", middle, backward_d)
    return (
        jnp.stack([resid_real, resid_imag], axis=1),
        jnp.stack([tile_out[0] * scale_sub, tile_out[1] * scale_sub], axis=1),
    )


def turn(value, modulus):
    angle = 2.0 * math.pi / modulus * (value % modulus).astype(F32)
    return jnp.cos(angle), jnp.sin(angle)


def split(value):
    high = lax.reduce_precision(value, 8, 7)
    return high.astype(BF16), (value - high).astype(BF16)


def split_in(value):
    high = value.astype(BF16)
    return high, (value - high.astype(F32)).astype(BF16)


def times_unit(pair, numerator, denominator):
    re, im = pair
    eighth = 8 * numerator % (8 * denominator)
    if eighth % denominator == 0:
        eighth //= denominator
        r = math.sqrt(0.5)
        if eighth == 0:
            return re, im
        if eighth == 2:
            return -im, re
        if eighth == 4:
            return -re, -im
        if eighth == 6:
            return im, -re
        if eighth == 1:
            return (re - im) * r, (re + im) * r
        if eighth == 3:
            return (re + im) * -r, (re - im) * r
        if eighth == 5:
            return (im - re) * r, (re + im) * -r
        return (re + im) * r, (im - re) * r
    angle = 2.0 * math.pi * (numerator % denominator) / denominator
    c, s = math.cos(angle), math.sin(angle)
    return re * c - im * s, re * s + im * c


def small_fft(values, sign):
    n = len(values)
    if n == 1:
        return values
    even, odd = small_fft(values[0::2], sign), small_fft(values[1::2], sign)
    out = [None] * n
    for k in range(n // 2):
        re, im = times_unit(odd[k], sign * k, n)
        out[k] = (even[k][0] + re, even[k][1] + im)
        out[k + n // 2] = (even[k][0] - re, even[k][1] - im)
    return out


def forward_kernel(
    tu_ref, image_ref, other_ref, dft2_ref, dft1_ref, turn_ref, col_ref, e_ref, out_ref,
    x_buf, z_buf, u_buf, lhs_buf, sems, *, ntile, blocks, chunk,
):
    step = pl.program_id(0)
    core = lax.rem(lax.axis_index("slab"), 2)
    kr = x_buf.shape[2]
    half = kr // 2
    per = SUB // kr
    tiles = ntile // 16

    def copies(block, slot):
        mine = pl.multiple_of(core * (blocks * LANES) + block * LANES, LANES)
        theirs = pl.multiple_of(block * LANES, LANES)
        return (
            pltpu.make_async_copy(
                image_ref.at[:, :, :, pl.ds(mine, LANES)],
                x_buf.at[slot, :, pl.ds(core * half, half)], sems.at[slot, 0]),
            pltpu.make_async_copy(
                other_ref.at[:, :, :, pl.ds(theirs, LANES)],
                x_buf.at[slot, :, pl.ds((1 - core) * half, half)], sems.at[slot, 1]),
        )

    @pl.when(step == 0)
    def _():
        for copy in copies(0, 0):
            copy.start()

        def one_block(block, carry):
            slot = lax.rem(block, 2)

            @pl.when(block + 1 < blocks)
            def _():
                for copy in copies(block + 1, 1 - slot):
                    copy.start()

            for copy in copies(block, slot):
                copy.wait()

            def rows(tile, carry):
                at = pl.ds(pl.multiple_of(tile * 16, 16), 16)
                turns = turn_ref[at, :]
                for q in range(per):
                    values = []
                    for k in range(kr):
                        pair = (x_buf[slot, 0, k, at, :], x_buf[slot, 1, k, at, :])
                        values.append(times_unit(pair, -q * k, SUB))
                    for m, (re, im) in enumerate(small_fft(values, -1)):
                        i = per * m + q
                        c = jnp.broadcast_to(turns[:, 2 * i:2 * i + 1], re.shape)
                        s = jnp.broadcast_to(turns[:, 2 * i + 1:2 * i + 2], re.shape)
                        lane = pl.ds(i % 2 * LANES, LANES)
                        for part, value in enumerate((re * c + im * s, im * c - re * s)):
                            high, low = split_in(value)
                            z_buf[i // 2, part, at, lane] = high
                            z_buf[i // 2, part + 2, at, lane] = low
                return carry

            lax.fori_loop(0, tiles, rows, 0)

            def pairs(pair, carry):
                z = z_buf[pair].reshape(4 * ntile, 2 * LANES)
                u = jnp.dot(dft2_ref[...], z, preferred_element_type=F32)
                u += jnp.dot(dft1_ref[...], z[:2 * ntile], preferred_element_type=F32)
                for part in range(2):
                    for side in range(2):
                        plane = pl.multiple_of((part * SUB + pair * 2 + side) * 8, 8)
                        u_buf[block, :, pl.ds(plane, 8), :] = u[
                            part * ntile:(part + 1) * ntile, side * LANES:(side + 1) * LANES
                        ].reshape(ntile // 8, 8, LANES)
                return carry

            lax.fori_loop(0, SUB // 2, pairs, 0)
            return carry

        lax.fori_loop(0, blocks, one_block, 0)

    wide = blocks * LANES

    def one(g, carry):
        tu = tu_ref[step * chunk + g]
        rows = pl.ds(pl.multiple_of(g * SUB, SUB), SUB)
        for block in range(blocks):
            x = u_buf[block, tu // 8, pl.ds(lax.rem(tu, 8), 2 * SUB, 8), :]
            c, s = e_ref[g, 2 * block:2 * block + 1, :], e_ref[g, 2 * block + 1:2 * block + 2, :]
            re, im = x[:SUB], x[SUB:]
            for part, value in enumerate((re * c + im * s, im * c - re * s)):
                high, low = split_in(value)
                lhs_buf[rows, pl.ds(part * wide + block * LANES, LANES)] = high
                lhs_buf[rows, pl.ds((part + 2) * wide + block * LANES, LANES)] = low
        return carry

    lax.fori_loop(0, chunk, one, 0, unroll=4)
    made = jnp.dot(lhs_buf[...], col_ref[...], preferred_element_type=F32)
    made = made + pltpu.roll(made, LANES // 2, 1)
    made = made.reshape(chunk, SUB, LANES)
    left = lax.broadcasted_iota(jnp.int32, (chunk, SUB // 2, LANES), 2) < LANES // 2
    out_ref[...] = jnp.where(left, made[:, :SUB // 2], made[:, SUB // 2:])


def backward_kernel(
    tu_ref, c_ref, dft2_ref, dft1_ref, turn_ref, col_ref, e_ref, image_ref, other_ref,
    x_buf, y_buf, s_buf, p_buf, sems, *, ntile, blocks, chunk, steps,
):
    step = pl.program_id(0)
    core = lax.rem(lax.axis_index("slab"), 2)
    kr = x_buf.shape[2]
    half = kr // 2
    per = SUB // kr
    wide = blocks * LANES

    @pl.when(step == 0)
    def _():
        zero = jnp.zeros((ntile // 8, 8, LANES), F32)

        def clear(plane, carry):
            for block in range(blocks):
                s_buf[block, :, pl.ds(pl.multiple_of(plane * 8, 8), 8), :] = zero
            return carry

        lax.fori_loop(0, 2 * SUB, clear, 0)

    given = c_ref[...]
    turned = pltpu.roll(given.reshape(chunk * SUB // 2, LANES), LANES // 2, 1).reshape(given.shape)
    left = lax.broadcasted_iota(jnp.int32, given.shape, 2) < LANES // 2
    both = jnp.concatenate([jnp.where(left, given, turned), jnp.where(left, turned, given)], axis=1)
    high, low = split_in(both.reshape(chunk * SUB, LANES))
    p_buf[...] = jnp.dot(jnp.concatenate([high, low], axis=1), col_ref[...], preferred_element_type=F32)

    def one(g, carry):
        tu = tu_ref[step * chunk + g]
        rows = pl.ds(pl.multiple_of(g * SUB, SUB), SUB)
        for block in range(blocks):
            re = p_buf[rows, pl.ds(block * LANES, LANES)]
            im = p_buf[rows, pl.ds(wide + block * LANES, LANES)]
            c, s = e_ref[g, 2 * block:2 * block + 1, :], e_ref[g, 2 * block + 1:2 * block + 2, :]
            at = pl.ds(lax.rem(tu, 8), 2 * SUB, 8)
            s_buf[block, tu // 8, at, :] = s_buf[block, tu // 8, at, :] + jnp.concatenate(
                [re * c - im * s, re * s + im * c], axis=0)
        return carry

    lax.fori_loop(0, chunk, one, 0, unroll=4)

    def copies(block, slot):
        mine = pl.multiple_of(core * wide + block * LANES, LANES)
        theirs = pl.multiple_of(block * LANES, LANES)
        return (
            pltpu.make_async_copy(
                x_buf.at[slot, :, pl.ds(core * half, half)],
                image_ref.at[:, :, :, pl.ds(mine, LANES)], sems.at[slot, 0]),
            pltpu.make_async_copy(
                x_buf.at[slot, :, pl.ds((1 - core) * half, half)],
                other_ref.at[:, :, :, pl.ds(theirs, LANES)], sems.at[slot, 1]),
        )

    @pl.when(step == steps - 1)
    def _():
        def one_block(block, carry):
            slot = lax.rem(block, 2)

            def pairs(pair, carry):
                parts = []
                for part in range(2):
                    sides = []
                    for side in range(2):
                        plane = pl.multiple_of((part * SUB + pair * 2 + side) * 8, 8)
                        sides.append(s_buf[block, :, pl.ds(plane, 8), :].reshape(ntile, LANES))
                    parts.append(jnp.concatenate(sides, axis=1))
                high, low = split_in(jnp.concatenate(parts, axis=0))
                y = jnp.dot(dft2_ref[...], jnp.concatenate([high, low], axis=0), preferred_element_type=F32)
                y += jnp.dot(dft1_ref[...], high, preferred_element_type=F32)
                for part in range(2):
                    for side in range(2):
                        y_buf[pair * 2 + side, part] = y[
                            part * ntile:(part + 1) * ntile, side * LANES:(side + 1) * LANES]
                return carry

            lax.fori_loop(0, SUB // 2, pairs, 0)

            @pl.when(block >= 2)
            def _():
                for copy in copies(block - 2, slot):
                    copy.wait()

            def rows(tile, carry):
                at = pl.ds(pl.multiple_of(tile * 8, 8), 8)
                turns = turn_ref[at, :]
                total = [None] * kr
                for q in range(per):
                    values = []
                    for m in range(kr):
                        i = per * m + q
                        re, im = y_buf[i, 0, at, :], y_buf[i, 1, at, :]
                        c = jnp.broadcast_to(turns[:, 2 * i:2 * i + 1], re.shape)
                        s = jnp.broadcast_to(turns[:, 2 * i + 1:2 * i + 2], re.shape)
                        values.append((re * c - im * s, re * s + im * c))
                    for k, value in enumerate(small_fft(values, 1)):
                        re, im = times_unit(value, q * k, SUB)
                        total[k] = (re, im) if q == 0 else (total[k][0] + re, total[k][1] + im)
                for k in range(kr):
                    x_buf[slot, 0, k, at, :] = total[k][0]
                    x_buf[slot, 1, k, at, :] = total[k][1]
                return carry

            lax.fori_loop(0, ntile // 8, rows, 0)
            for copy in copies(block, slot):
                copy.start()
            return carry

        lax.fori_loop(0, blocks, one_block, 0)
        for block in range(max(0, blocks - 2), blocks):
            for copy in copies(block, block % 2):
                copy.wait()


MESH = pl.DeviceIdType.MESH


def greet(peers):
    barrier = pltpu.get_barrier_semaphore()
    for peer in peers:
        pl.semaphore_signal(barrier, inc=1, device_id=peer, device_id_type=MESH)
    pl.semaphore_wait(barrier, len(peers))


def swap_kernel(ids_ref, image_ref, other_ref, all_ref, send_sem, recv_sem, id_send, id_recv, *, bands, groups):
    slab, bl = lax.axis_index("slab"), lax.axis_index("bl")
    core = lax.rem(slab, 2)
    count = bands * groups
    me = slab * groups + bl
    wide = other_ref.shape[-1]
    barrier = pltpu.get_barrier_semaphore()

    def peer(offset):
        to = lax.rem(me + offset, count)
        return (to // groups, lax.rem(to, groups))

    def hello(offset, carry):
        pl.semaphore_signal(barrier, inc=1, device_id=peer(offset), device_id_type=MESH)
        return carry

    lax.fori_loop(1, count, hello, 0)
    pl.semaphore_wait(barrier, count - 1)

    partner = (slab + 1 - 2 * core, bl)
    away = pl.multiple_of((1 - core) * wide, LANES)
    swaps = []
    for part in range(image_ref.shape[0]):
        for k in range(image_ref.shape[1]):
            swaps.append(pltpu.make_async_remote_copy(
                src_ref=image_ref.at[part, k, :, pl.ds(away, wide)],
                dst_ref=other_ref.at[part, k],
                send_sem=send_sem.at[part, k], recv_sem=recv_sem.at[part, k],
                device_id=partner, device_id_type=MESH))

    def tell(offset):
        return pltpu.make_async_remote_copy(
            src_ref=ids_ref, dst_ref=all_ref.at[me],
            send_sem=id_send.at[offset], recv_sem=id_recv.at[offset],
            device_id=peer(offset), device_id_type=MESH)

    def start(offset, carry):
        tell(offset).start()
        return carry

    def finish(offset, carry):
        tell(offset).wait()
        return carry

    for swap in swaps:
        swap.start()
    lax.fori_loop(1, count, start, 0)
    all_ref[me] = ids_ref[...]
    lax.fori_loop(1, count, finish, 0)
    for swap in swaps:
        swap.wait()


class Grid:
    def __init__(self, sizes):
        self.sizes = sizes
        self.slab, self.bl = lax.axis_index("slab"), lax.axis_index("bl")
        self.y, self.core = self.slab // 2, lax.rem(self.slab, 2)
        self.z, self.x = self.bl // sizes["x"], lax.rem(self.bl, sizes["x"])

    def along(self, axis, offset):
        if axis == "core":
            return (self.slab + 1 - 2 * self.core, self.bl)
        at = lax.rem(getattr(self, axis) + offset, self.sizes[axis])
        if axis == "y":
            return (at * 2 + self.core, self.bl)
        if axis == "z":
            return (self.slab, at * self.sizes["x"] + self.x)
        return (self.slab, self.z * self.sizes["x"] + at)

    def others(self):
        peers = [self.along("core", 1)]
        for axis in "yzx":
            peers += [self.along(axis, offset) for offset in range(1, self.sizes[axis])]
        return peers


def send(src, dst, sems, at, to):
    copy = pltpu.make_async_remote_copy(
        src_ref=src, dst_ref=dst, send_sem=sems.at[(0,) + at], recv_sem=sems.at[(1,) + at],
        device_id=to, device_id_type=MESH)
    copy.start()
    return copy


def reduce_kernel(
    part_ref, out_ref, r0, c0, r1a, c1a, r1b, c1b, r2a, r2b, c2, r3,
    s_own, s0, s1a, s1b, s2a, s2b, s3, *, sizes,
):
    place = Grid(sizes)
    ny, nz, nx = sizes["y"], sizes["z"], sizes["x"]
    x, y, z, core = place.x, place.y, place.z, place.core
    greet(place.others())
    owns, first = [], []
    for h in range(2):
        first.append(send(part_ref.at[:, 1 - core, :, :, h], r0.at[h], s0, (h,), place.along("core", 1)))
    for h in range(2):
        own = pltpu.make_async_copy(part_ref.at[:, core, :, :, h], c0.at[h], s_own.at[h])
        own.start()
        owns.append(own)

    def total(h):
        owns[h].wait()
        first[h].wait_recv()

        def add(at, carry):
            iy, iz, ix = at // (nz * nx), lax.rem(at // nx, nz), lax.rem(at, nx)
            c0[h, iy, iz, ix] = c0[h, iy, iz, ix] + r0[h, iy, iz, ix]
            return carry

        lax.fori_loop(0, ny * nz * nx, add, 0)

    def summed(value, got, *at):
        for o in range(got.shape[0]):
            value = value + got[(o,) + at]
        return value

    total(0)
    one_a = [send(c0.at[0, lax.rem(y + o, ny)], r1a.at[o - 1], s1a, (o - 1,), place.along("y", o))
             for o in range(1, ny)]
    total(1)
    one_b = [send(c0.at[1, :, :, lax.rem(x + o, nx)], r1b.at[o - 1], s1b, (o - 1,), place.along("x", o))
             for o in range(1, nx)]
    for copy in one_a:
        copy.wait_recv()

    def add_one_a(at, carry):
        iz, ix = at // nx, lax.rem(at, nx)
        c1a[iz, ix] = summed(c0[0, y, iz, ix], r1a, iz, ix)
        return carry

    lax.fori_loop(0, nz * nx, add_one_a, 0)
    two_a = [send(c1a.at[:, lax.rem(x + o, nx)], r2a.at[o - 1], s2a, (o - 1,), place.along("x", o))
             for o in range(1, nx)]
    for copy in one_b:
        copy.wait_recv()

    def add_one_b(at, carry):
        iy, iz = at // nz, lax.rem(at, nz)
        c1b[iy, iz] = summed(c0[1, iy, iz, x], r1b, iy, iz)
        return carry

    lax.fori_loop(0, ny * nz, add_one_b, 0)
    two_b = [send(c1b.at[lax.rem(y + o, ny)], r2b.at[o - 1], s2b, (o - 1,), place.along("y", o))
             for o in range(1, ny)]
    three = []
    for h, copies in enumerate((two_a, two_b)):
        for copy in copies:
            copy.wait_recv()

        def add_two(iz, carry):
            c2[h, iz] = summed(c1a[iz, x], r2a, iz) if h == 0 else summed(c1b[y, iz], r2b, iz)
            return carry

        lax.fori_loop(0, nz, add_two, 0)
        three.append([
            send(c2.at[h, lax.rem(z + o, nz)], r3.at[h, o - 1], s3, (h, o - 1), place.along("z", o))
            for o in range(1, nz)])
    for h in range(2):
        for copy in three[h]:
            copy.wait_recv()
        value = c2[h, z]
        for o in range(nz - 1):
            value = value + r3[h, o]
        out_ref[h] = value
    for copy in first + one_a + one_b + two_a + two_b + three[0] + three[1]:
        copy.wait_send()


def gather_kernel(mine_ref, out_ref, s_own, s_z, s_two, s_three, s_core, *, sizes):
    place = Grid(sizes)
    x, y, z, core = place.x, place.y, place.z, place.core
    greet(place.others())
    own = pltpu.make_async_copy(mine_ref, out_ref.at[y, core, z, x], s_own)
    own.start()
    along_z = [
        [send(mine_ref.at[h], out_ref.at[y, core, z, x, h], s_z, (h, o - 1), place.along("z", o))
         for o in range(1, sizes["z"])] for h in range(2)]
    own.wait()
    two = []
    for h, axis in enumerate("xy"):
        for copy in along_z[h]:
            copy.wait_recv()
        ref = out_ref.at[y, core, :, x, h]
        two.append([send(ref, ref, s_two, (h, o - 1), place.along(axis, o)) for o in range(1, sizes[axis])])
    three = []
    for h, axis in enumerate("yx"):
        for copy in two[h]:
            copy.wait_recv()
        ref = out_ref.at[y, core, :, :, 0] if h == 0 else out_ref.at[:, core, :, x, 1]
        three.append([send(ref, ref, s_three, (h, o - 1), place.along(axis, o)) for o in range(1, sizes[axis])])
    last = []
    for h in range(2):
        for copy in three[h]:
            copy.wait_recv()
        ref = out_ref.at[:, core, :, :, h]
        last.append(send(ref, ref, s_core, (h,), place.along("core", 1)))
    for copy in last:
        copy.wait_recv()
    for copy in along_z[0] + along_z[1] + two[0] + two[1] + three[0] + three[1] + last:
        copy.wait_send()


def talk(number):
    return pltpu.CompilerParams(collective_id=number, has_side_effects=True, vmem_limit_bytes=67_000_000)


def swap_and_name(image, ids, bands, groups):
    halves, wide = image.shape[:3], image.shape[3] // 2
    count = bands * groups
    return pl.pallas_call(
        functools.partial(swap_kernel, bands=bands, groups=groups),
        in_specs=[pl.BlockSpec(memory_space=pltpu.VMEM), pl.BlockSpec(memory_space=pl.ANY)],
        out_specs=[pl.BlockSpec(memory_space=pl.ANY), pl.BlockSpec(memory_space=pltpu.VMEM)],
        out_shape=[
            jax.ShapeDtypeStruct(halves + (wide,), F32),
            jax.ShapeDtypeStruct((count,) + ids.shape, jnp.int32),
        ],
        scratch_shapes=[
            pltpu.SemaphoreType.DMA(halves[:2]), pltpu.SemaphoreType.DMA(halves[:2]),
            pltpu.SemaphoreType.DMA((count,)), pltpu.SemaphoreType.DMA((count,)),
        ],
        compiler_params=talk(1),
        name="swap_columns",
    )(ids, image)


def grid_sizes(bands, groups):
    ny = bands // 2
    nx = math.gcd(groups, ny)
    return {"y": ny, "x": nx, "z": groups // nx}


def reduce_tiles(partial, bands, groups):
    sizes = grid_sizes(bands, groups)
    ny, nz, nx = sizes["y"], sizes["z"], sizes["x"]
    total, rows = partial.shape[:2]
    block = (total // (bands * groups) // 2 * rows, LANES)
    vmem = lambda *shape: pltpu.VMEM(shape + block, F32)
    sems = lambda *shape: pltpu.SemaphoreType.DMA((2,) + tuple(max(1, n) for n in shape))
    out = pl.pallas_call(
        functools.partial(reduce_kernel, sizes=sizes),
        in_specs=[pl.BlockSpec(memory_space=pl.ANY)],
        out_specs=pl.BlockSpec(memory_space=pltpu.VMEM),
        out_shape=jax.ShapeDtypeStruct((2,) + block, F32),
        scratch_shapes=[
            vmem(2, ny, nz, nx), vmem(2, ny, nz, nx),
            vmem(ny - 1, nz, nx), vmem(nz, nx),
            vmem(nx - 1, ny, nz), vmem(ny, nz),
            vmem(nx - 1, nz), vmem(ny - 1, nz), vmem(2, nz), vmem(2, nz - 1),
            pltpu.SemaphoreType.DMA((2,)), sems(2), sems(ny - 1), sems(nx - 1),
            sems(nx - 1), sems(ny - 1), sems(2, nz - 1),
        ],
        compiler_params=talk(2),
        name="reduce_tiles",
    )(partial.reshape((ny, 2, nz, nx, 2) + block))
    return out.reshape(total // (bands * groups), rows, LANES)


def gather_tiles(mine, bands, groups):
    sizes = grid_sizes(bands, groups)
    ny, nz, nx = sizes["y"], sizes["z"], sizes["x"]
    count, rows = mine.shape[:2]
    block = (count // 2 * rows, LANES)
    most = max(nx, ny) - 1
    sems = lambda *shape: pltpu.SemaphoreType.DMA((2,) + shape)
    out = pl.pallas_call(
        functools.partial(gather_kernel, sizes=sizes),
        in_specs=[pl.BlockSpec(memory_space=pltpu.VMEM)],
        out_specs=pl.BlockSpec(memory_space=pl.ANY),
        out_shape=jax.ShapeDtypeStruct((ny, 2, nz, nx, 2) + block, F32),
        scratch_shapes=[
            pltpu.SemaphoreType.DMA, sems(2, nz - 1), sems(2, most), sems(2, most), sems(2),
        ],
        compiler_params=talk(3),
        name="gather_tiles",
    )(mine.reshape((2,) + block))
    return out.reshape(bands * groups * count, rows, LANES)


def complex_table(cos, sin):
    return jnp.concatenate(
        [jnp.concatenate([cos, -sin], axis=1), jnp.concatenate([sin, cos], axis=1)], axis=0)


def per_device(model_image, vis_coords, vis_observed, tile_slot, tile_group, w_plane, vis_count):
    groups = lax.axis_size("bl")
    bands = lax.axis_size("slab")
    rows, cols = model_image.shape[1:]
    length = rows * bands
    ntile = length // SUB
    band = lax.axis_index("slab")
    core = lax.rem(band, 2)
    wide = cols // 2
    blocks = wide // LANES
    kr = 2 * rows // ntile
    swap = [(d, d ^ 1) for d in range(bands)]

    sub_count = tile_slot.shape[0]
    tile_cols = ntile // (bands * groups)
    own_tv = (band * groups + tile_group[:, 0]) * tile_cols + tile_slot // ntile
    own_tu = tile_slot % ntile
    ids = jnp.pad(jnp.stack([own_tu, own_tv]), ((0, 6), (0, LANES - sub_count)))
    shaped = model_image.reshape(2, kr // 2, ntile, cols)
    other, named = swap_and_name(shaped, ids, bands, groups)
    tu = named[:, 0, :sub_count].reshape(-1)
    tv = named[:, 1, :sub_count].reshape(-1)
    total = tu.shape[0]
    chunk = math.gcd(total, 32)
    steps = total // chunk

    inner = jnp.arange(ntile, dtype=jnp.int32)
    outer = jnp.arange(SUB, dtype=jnp.int32)
    own_cols = lax.axis_index("bl") * cols + core * wide + jnp.arange(wide, dtype=jnp.int32)
    first_row = band // 2 * (2 * rows)

    dft_c, dft_s = turn(inner[:, None] * inner[None, :], ntile)
    fwd_high, fwd_low = split(complex_table(dft_c, -dft_s))
    bwd_high, bwd_low = split(complex_table(dft_c, dft_s))
    turns = jnp.stack(turn((first_row + inner)[:, None] * outer[None, :], length), axis=2)
    turns = jnp.pad(turns.reshape(ntile, 2 * SUB), ((0, 0), (0, LANES - 2 * SUB)))
    col_c, col_s = turn(own_cols[:, None] * outer[None, :], length)
    col_c, col_s = col_c / length, col_s / length
    out_high, out_low = split(jnp.concatenate(
        [jnp.concatenate([col_c, -col_s], axis=1), jnp.concatenate([col_s, col_c], axis=1)], axis=0))
    zero = jnp.zeros_like(out_high)
    col_fwd = jnp.concatenate(
        [jnp.concatenate([out_high, out_low], axis=1), jnp.concatenate([out_high, zero], axis=1)], axis=0)
    in_high, in_low = split(jnp.concatenate(
        [jnp.concatenate([col_c.T, col_s.T], axis=1), jnp.concatenate([-col_s.T, col_c.T], axis=1)], axis=0))
    col_bwd = jnp.concatenate([in_high, in_low, in_high, in_low], axis=0)
    e_c, e_s = turn(tv[:, None] * own_cols[None, :], ntile)
    e_table = jnp.stack([e_c.reshape(total, blocks, LANES), e_s.reshape(total, blocks, LANES)], axis=2)
    e_table = e_table.reshape(total, 2 * blocks, LANES)

    whole = lambda shape: pl.BlockSpec(shape, lambda step, ids: (0,) * len(shape))
    by_step = lambda shape: pl.BlockSpec(shape, lambda step, ids: (step,) + (0,) * (len(shape) - 1))
    anywhere = pl.BlockSpec(memory_space=pl.ANY)
    params = pltpu.CompilerParams(
        dimension_semantics=("arbitrary",), vmem_limit_bytes=67_000_000)
    partial = pl.pallas_call(
        functools.partial(forward_kernel, ntile=ntile, blocks=blocks, chunk=chunk),
        grid_spec=pltpu.PrefetchScalarGridSpec(
            num_scalar_prefetch=1,
            grid=(steps,),
            in_specs=[
                anywhere, anywhere,
                whole((2 * ntile, 4 * ntile)), whole((2 * ntile, 2 * ntile)), whole((ntile, LANES)),
                whole((4 * wide, LANES)), by_step((chunk, 2 * blocks, LANES)),
            ],
            out_specs=by_step((chunk, SUB // 2, LANES)),
            scratch_shapes=[
                pltpu.VMEM((2, 2, kr, ntile, LANES), F32),
                pltpu.VMEM((SUB // 2, 4, ntile, 2 * LANES), BF16),
                pltpu.VMEM((blocks, ntile // 8, 2 * SUB * 8, LANES), F32),
                pltpu.VMEM((chunk * SUB, 4 * wide), BF16),
                pltpu.SemaphoreType.DMA((2, 2)),
            ],
        ),
        out_shape=jax.ShapeDtypeStruct((total, SUB // 2, LANES), F32),
        compiler_params=params,
        name="tiles_from_image",
    )(
        tu,
        shaped, other,
        jnp.concatenate([fwd_high, fwd_high], axis=1), fwd_low, turns, col_fwd, e_table,
    )
    mine = reduce_tiles(partial, bands, groups)
    mine = mine.reshape(sub_count, SUB // 2, 2, 2, SUB).transpose(3, 0, 2, 1, 4)
    mine = mine.reshape(2, sub_count, SUB, SUB)
    residual_vis, contrib = subgrid_pass(
        mine[0], mine[1], vis_coords, vis_observed, w_plane, vis_count)
    contrib = contrib.reshape(sub_count, 2, 2, SUB // 2, SUB).transpose(0, 3, 2, 1, 4)
    everyone = gather_tiles(contrib.reshape(sub_count, SUB // 2, LANES), bands, groups)

    image, leaving = pl.pallas_call(
        functools.partial(backward_kernel, ntile=ntile, blocks=blocks, chunk=chunk, steps=steps),
        grid_spec=pltpu.PrefetchScalarGridSpec(
            num_scalar_prefetch=1,
            grid=(steps,),
            in_specs=[
                by_step((chunk, SUB // 2, LANES)),
                whole((2 * ntile, 4 * ntile)), whole((2 * ntile, 2 * ntile)), whole((ntile, LANES)),
                whole((8 * SUB, 2 * wide)), by_step((chunk, 2 * blocks, LANES)),
            ],
            out_specs=[anywhere, anywhere],
            scratch_shapes=[
                pltpu.VMEM((2, 2, kr, ntile, LANES), F32),
                pltpu.VMEM((SUB, 2, ntile, LANES), F32),
                pltpu.VMEM((blocks, ntile // 8, 2 * SUB * 8, LANES), F32),
                pltpu.VMEM((chunk * SUB, 2 * wide), F32),
                pltpu.SemaphoreType.DMA((2, 2)),
            ],
        ),
        out_shape=[
            jax.ShapeDtypeStruct((2, kr // 2, ntile, cols), F32),
            jax.ShapeDtypeStruct((2, kr // 2, ntile, wide), F32),
        ],
        compiler_params=params,
        name="image_from_tiles",
    )(
        tu, everyone,
        jnp.concatenate([bwd_high, bwd_high], axis=1), bwd_low, turns, col_bwd, e_table,
    )
    arrived = lax.ppermute(leaving.reshape(2, rows, wide), "slab", swap)
    image = lax.dynamic_update_slice_in_dim(
        image.reshape(2, rows, cols), arrived, (1 - core) * wide, axis=2)
    return (image, residual_vis)


def solution(mesh):
    placed = (
        P(None, "slab", "bl"),
        P(("slab", "bl"), None, None),
        P(("slab", "bl"), None, None),
        P(("slab", "bl")),
        P(("slab", "bl"), None),
        P(("slab", "bl")),
        P(("slab", "bl")),
    )
    return jax.shard_map(
        per_device,
        mesh=mesh,
        in_specs=placed,
        out_specs=(P(None, "slab", "bl"), P(("slab", "bl"), None, None)),
        check_vma=False,
    )
```

```python
import functools
import math

import jax
import jax.numpy as jnp
import numpy as np
from jax import lax
from jax.experimental import pallas as pl
from jax.experimental.pallas import tpu as pltpu
from jax.sharding import PartitionSpec as P

SUB = 32
LANES = 128
F32, BF16 = jnp.float32, jnp.bfloat16

w_step = 0.1


def complex_einsum(form, left, right):
    names, made = form.split("->")
    first, second = names.split(",")
    re, im = right
    table = jnp.stack([jnp.stack([re, im]), jnp.stack([-im, re])])
    out = jnp.einsum(
        f"P{first},PQ{second}->Q{made}", jnp.stack(left), table, precision=lax.Precision.HIGH)
    return out[0], out[1]


def complex_mul(left, right):
    return (left[0] * right[0] - left[1] * right[1], left[0] * right[1] + left[1] * right[0])


def subgrid_pass(tile_real, tile_imag, coords, observed, planes, counts):
    width = tile_real.shape[-1]
    half = width // 2
    slots = coords.shape[-1]
    index = jnp.arange(width, dtype=jnp.int32)
    offsets = (index - half).astype(jnp.float32)
    turns = index[:, None] * (index[None, :] - half) % width
    angle = 2.0 * math.pi / width * turns.astype(jnp.float32)
    forward_d = (jnp.cos(angle), jnp.sin(angle))
    backward_d = (forward_d[0], -forward_d[1])
    scale_sub = 1.0 / (width * width)
    halfway = complex_einsum("il,kij->klj", forward_d, (tile_real, tile_imag))
    image_sub = complex_einsum("klj,jm->klm", halfway, forward_d)
    image_sub = (image_sub[0] * scale_sub, image_sub[1] * scale_sub)
    radius = (offsets[:, None] ** 2 + offsets[None, :] ** 2) / (half * half)
    phase = -w_step * planes.astype(jnp.float32)[:, None, None] * radius[None]
    screen = (jnp.cos(phase), jnp.sin(phase))
    weighted = complex_mul(screen, image_sub)
    along_a = -2.0 * math.pi / width * coords[:, 0, :][:, None, :] * offsets[None, :, None]
    along_b = -2.0 * math.pi / width * coords[:, 1, :][:, None, :] * offsets[None, :, None]
    phase_a = (jnp.cos(along_a), jnp.sin(along_a))
    phase_b = (jnp.cos(along_b), jnp.sin(along_b))
    partial_rows = complex_einsum("klm,kmj->klj", weighted, phase_b)
    terms = complex_mul(phase_a, partial_rows)
    predicted = (jnp.sum(terms[0], axis=1), jnp.sum(terms[1], axis=1))
    live = (jnp.arange(slots, dtype=jnp.int32)[None, :] < counts[:, None]).astype(jnp.float32)
    resid_real = (observed[:, 0, :] - predicted[0]) * live
    resid_imag = (observed[:, 1, :] - predicted[1]) * live
    spread = complex_mul(
        (phase_a[0], -phase_a[1]), (resid_real[:, None, :], resid_imag[:, None, :])
    )
    collected = complex_einsum("klj,kmj->klm", spread, (phase_b[0], -phase_b[1]))
    unscreened = complex_mul((screen[0], -screen[1]), collected)
    middle = complex_einsum("il,klm->kim", backward_d, unscreened)
    tile_out = complex_einsum("kim,jm->kij", middle, backward_d)
    return (
        jnp.stack([resid_real, resid_imag], axis=1),
        jnp.stack([tile_out[0] * scale_sub, tile_out[1] * scale_sub], axis=1),
    )


def turn(value, modulus):
    angle = 2.0 * math.pi / modulus * (value % modulus).astype(F32)
    return jnp.cos(angle), jnp.sin(angle)


def split(value):
    high = lax.reduce_precision(value, 8, 7)
    return high.astype(BF16), (value - high).astype(BF16)


def split_in(value):
    high = value.astype(BF16)
    return high, (value - high.astype(F32)).astype(BF16)


def times_unit(pair, numerator, denominator):
    re, im = pair
    eighth = 8 * numerator % (8 * denominator)
    if eighth % denominator == 0:
        eighth //= denominator
        r = math.sqrt(0.5)
        if eighth == 0:
            return re, im
        if eighth == 2:
            return -im, re
        if eighth == 4:
            return -re, -im
        if eighth == 6:
            return im, -re
        if eighth == 1:
            return (re - im) * r, (re + im) * r
        if eighth == 3:
            return (re + im) * -r, (re - im) * r
        if eighth == 5:
            return (im - re) * r, (re + im) * -r
        return (re + im) * r, (im - re) * r
    angle = 2.0 * math.pi * (numerator % denominator) / denominator
    c, s = math.cos(angle), math.sin(angle)
    return re * c - im * s, re * s + im * c


def small_fft(values, sign):
    n = len(values)
    if n == 1:
        return values
    even, odd = small_fft(values[0::2], sign), small_fft(values[1::2], sign)
    out = [None] * n
    for k in range(n // 2):
        re, im = times_unit(odd[k], sign * k, n)
        out[k] = (even[k][0] + re, even[k][1] + im)
        out[k + n // 2] = (even[k][0] - re, even[k][1] - im)
    return out


def forward_kernel(
    tu_ref, image_ref, other_ref, dft2_ref, dft1_ref, turn_ref, col_ref, e_ref, out_ref,
    x_buf, z_buf, u_buf, lhs_buf, sems, *, ntile, blocks, chunk,
):
    step = pl.program_id(0)
    core = lax.rem(lax.axis_index("slab"), 2)
    kr = x_buf.shape[2]
    half = kr // 2
    per = SUB // kr
    tiles = ntile // 16

    def copies(block, slot):
        mine = pl.multiple_of(core * (blocks * LANES) + block * LANES, LANES)
        theirs = pl.multiple_of(block * LANES, LANES)
        return (
            pltpu.make_async_copy(
                image_ref.at[:, :, :, pl.ds(mine, LANES)],
                x_buf.at[slot, :, pl.ds(core * half, half)], sems.at[slot, 0]),
            pltpu.make_async_copy(
                other_ref.at[:, :, :, pl.ds(theirs, LANES)],
                x_buf.at[slot, :, pl.ds((1 - core) * half, half)], sems.at[slot, 1]),
        )

    @pl.when(step == 0)
    def _():
        for copy in copies(0, 0):
            copy.start()

        def one_block(block, carry):
            slot = lax.rem(block, 2)

            @pl.when(block + 1 < blocks)
            def _():
                for copy in copies(block + 1, 1 - slot):
                    copy.start()

            for copy in copies(block, slot):
                copy.wait()

            def rows(tile, carry):
                at = pl.ds(pl.multiple_of(tile * 16, 16), 16)
                turns = turn_ref[at, :]
                for q in range(per):
                    values = []
                    for k in range(kr):
                        pair = (x_buf[slot, 0, k, at, :], x_buf[slot, 1, k, at, :])
                        values.append(times_unit(pair, -q * k, SUB))
                    for m, (re, im) in enumerate(small_fft(values, -1)):
                        i = per * m + q
                        c = jnp.broadcast_to(turns[:, 2 * i:2 * i + 1], re.shape)
                        s = jnp.broadcast_to(turns[:, 2 * i + 1:2 * i + 2], re.shape)
                        lane = pl.ds(i % 2 * LANES, LANES)
                        for part, value in enumerate((re * c + im * s, im * c - re * s)):
                            high, low = split_in(value)
                            z_buf[i // 2, part, at, lane] = high
                            z_buf[i // 2, part + 2, at, lane] = low
                return carry

            lax.fori_loop(0, tiles, rows, 0)

            def pairs(pair, carry):
                z = z_buf[pair].reshape(4 * ntile, 2 * LANES)
                u = jnp.dot(dft2_ref[...], z, preferred_element_type=F32)
                u += jnp.dot(dft1_ref[...], z[:2 * ntile], preferred_element_type=F32)
                for part in range(2):
                    for side in range(2):
                        plane = pl.multiple_of((part * SUB + pair * 2 + side) * 8, 8)
                        u_buf[block, :, pl.ds(plane, 8), :] = u[
                            part * ntile:(part + 1) * ntile, side * LANES:(side + 1) * LANES
                        ].reshape(ntile // 8, 8, LANES)
                return carry

            lax.fori_loop(0, SUB // 2, pairs, 0)
            return carry

        lax.fori_loop(0, blocks, one_block, 0)

    wide = blocks * LANES

    def one(g, carry):
        tu = tu_ref[step * chunk + g]
        rows = pl.ds(pl.multiple_of(g * SUB, SUB), SUB)
        for block in range(blocks):
            x = u_buf[block, tu // 8, pl.ds(lax.rem(tu, 8), 2 * SUB, 8), :]
            c, s = e_ref[g, 2 * block:2 * block + 1, :], e_ref[g, 2 * block + 1:2 * block + 2, :]
            re, im = x[:SUB], x[SUB:]
            for part, value in enumerate((re * c + im * s, im * c - re * s)):
                high, low = split_in(value)
                lhs_buf[rows, pl.ds(part * wide + block * LANES, LANES)] = high
                lhs_buf[rows, pl.ds((part + 2) * wide + block * LANES, LANES)] = low
        return carry

    lax.fori_loop(0, chunk, one, 0, unroll=4)
    made = jnp.dot(lhs_buf[...], col_ref[...], preferred_element_type=F32)
    made = made + pltpu.roll(made, LANES // 2, 1)
    made = made.reshape(chunk, SUB, LANES)
    left = lax.broadcasted_iota(jnp.int32, (chunk, SUB // 2, LANES), 2) < LANES // 2
    out_ref[...] = jnp.where(left, made[:, :SUB // 2], made[:, SUB // 2:])


def backward_kernel(
    tu_ref, c_ref, dft2_ref, dft1_ref, turn_ref, col_ref, e_ref, image_ref, other_ref,
    x_buf, y_buf, s_buf, p_buf, sems, *, ntile, blocks, chunk, steps,
):
    step = pl.program_id(0)
    core = lax.rem(lax.axis_index("slab"), 2)
    kr = x_buf.shape[2]
    half = kr // 2
    per = SUB // kr
    wide = blocks * LANES

    @pl.when(step == 0)
    def _():
        zero = jnp.zeros((ntile // 8, 8, LANES), F32)

        def clear(plane, carry):
            for block in range(blocks):
                s_buf[block, :, pl.ds(pl.multiple_of(plane * 8, 8), 8), :] = zero
            return carry

        lax.fori_loop(0, 2 * SUB, clear, 0)

    given = c_ref[...]
    turned = pltpu.roll(given.reshape(chunk * SUB // 2, LANES), LANES // 2, 1).reshape(given.shape)
    left = lax.broadcasted_iota(jnp.int32, given.shape, 2) < LANES // 2
    both = jnp.concatenate([jnp.where(left, given, turned), jnp.where(left, turned, given)], axis=1)
    high, low = split_in(both.reshape(chunk * SUB, LANES))
    p_buf[...] = jnp.dot(jnp.concatenate([high, low], axis=1), col_ref[...], preferred_element_type=F32)

    def one(g, carry):
        tu = tu_ref[step * chunk + g]
        rows = pl.ds(pl.multiple_of(g * SUB, SUB), SUB)
        for block in range(blocks):
            re = p_buf[rows, pl.ds(block * LANES, LANES)]
            im = p_buf[rows, pl.ds(wide + block * LANES, LANES)]
            c, s = e_ref[g, 2 * block:2 * block + 1, :], e_ref[g, 2 * block + 1:2 * block + 2, :]
            at = pl.ds(lax.rem(tu, 8), 2 * SUB, 8)
            s_buf[block, tu // 8, at, :] = s_buf[block, tu // 8, at, :] + jnp.concatenate(
                [re * c - im * s, re * s + im * c], axis=0)
        return carry

    lax.fori_loop(0, chunk, one, 0, unroll=4)

    def copies(block, slot):
        mine = pl.multiple_of(core * wide + block * LANES, LANES)
        theirs = pl.multiple_of(block * LANES, LANES)
        return (
            pltpu.make_async_copy(
                x_buf.at[slot, :, pl.ds(core * half, half)],
                image_ref.at[:, :, :, pl.ds(mine, LANES)], sems.at[slot, 0]),
            pltpu.make_async_copy(
                x_buf.at[slot, :, pl.ds((1 - core) * half, half)],
                other_ref.at[:, :, :, pl.ds(theirs, LANES)], sems.at[slot, 1]),
        )

    @pl.when(step == steps - 1)
    def _():
        def one_block(block, carry):
            slot = lax.rem(block, 2)

            def pairs(pair, carry):
                parts = []
                for part in range(2):
                    sides = []
                    for side in range(2):
                        plane = pl.multiple_of((part * SUB + pair * 2 + side) * 8, 8)
                        sides.append(s_buf[block, :, pl.ds(plane, 8), :].reshape(ntile, LANES))
                    parts.append(jnp.concatenate(sides, axis=1))
                high, low = split_in(jnp.concatenate(parts, axis=0))
                y = jnp.dot(dft2_ref[...], jnp.concatenate([high, low], axis=0), preferred_element_type=F32)
                y += jnp.dot(dft1_ref[...], high, preferred_element_type=F32)
                for part in range(2):
                    for side in range(2):
                        y_buf[pair * 2 + side, part] = y[
                            part * ntile:(part + 1) * ntile, side * LANES:(side + 1) * LANES]
                return carry

            lax.fori_loop(0, SUB // 2, pairs, 0)

            @pl.when(block >= 2)
            def _():
                for copy in copies(block - 2, slot):
                    copy.wait()

            def rows(tile, carry):
                at = pl.ds(pl.multiple_of(tile * 8, 8), 8)
                turns = turn_ref[at, :]
                total = [None] * kr
                for q in range(per):
                    values = []
                    for m in range(kr):
                        i = per * m + q
                        re, im = y_buf[i, 0, at, :], y_buf[i, 1, at, :]
                        c = jnp.broadcast_to(turns[:, 2 * i:2 * i + 1], re.shape)
                        s = jnp.broadcast_to(turns[:, 2 * i + 1:2 * i + 2], re.shape)
                        values.append((re * c - im * s, re * s + im * c))
                    for k, value in enumerate(small_fft(values, 1)):
                        re, im = times_unit(value, q * k, SUB)
                        total[k] = (re, im) if q == 0 else (total[k][0] + re, total[k][1] + im)
                for k in range(kr):
                    x_buf[slot, 0, k, at, :] = total[k][0]
                    x_buf[slot, 1, k, at, :] = total[k][1]
                return carry

            lax.fori_loop(0, ntile // 8, rows, 0)
            for copy in copies(block, slot):
                copy.start()
            return carry

        lax.fori_loop(0, blocks, one_block, 0)
        for block in range(max(0, blocks - 2), blocks):
            for copy in copies(block, block % 2):
                copy.wait()


MESH = pl.DeviceIdType.MESH


def greet(peers):
    barrier = pltpu.get_barrier_semaphore()
    for peer in peers:
        pl.semaphore_signal(barrier, inc=1, device_id=peer, device_id_type=MESH)
    pl.semaphore_wait(barrier, len(peers))


def swap_kernel(ids_ref, image_ref, other_ref, all_ref, send_sem, recv_sem, id_send, id_recv, *, bands, groups):
    slab, bl = lax.axis_index("slab"), lax.axis_index("bl")
    core = lax.rem(slab, 2)
    count = bands * groups
    me = slab * groups + bl
    wide = other_ref.shape[-1]
    barrier = pltpu.get_barrier_semaphore()

    def peer(offset):
        to = lax.rem(me + offset, count)
        return (to // groups, lax.rem(to, groups))

    def hello(offset, carry):
        pl.semaphore_signal(barrier, inc=1, device_id=peer(offset), device_id_type=MESH)
        return carry

    lax.fori_loop(1, count, hello, 0)
    pl.semaphore_wait(barrier, count - 1)

    partner = (slab + 1 - 2 * core, bl)
    away = pl.multiple_of((1 - core) * wide, LANES)
    swaps = []
    for part in range(image_ref.shape[0]):
        for k in range(image_ref.shape[1]):
            swaps.append(pltpu.make_async_remote_copy(
                src_ref=image_ref.at[part, k, :, pl.ds(away, wide)],
                dst_ref=other_ref.at[part, k],
                send_sem=send_sem.at[part, k], recv_sem=recv_sem.at[part, k],
                device_id=partner, device_id_type=MESH))

    def tell(offset):
        return pltpu.make_async_remote_copy(
            src_ref=ids_ref, dst_ref=all_ref.at[me],
            send_sem=id_send.at[offset], recv_sem=id_recv.at[offset],
            device_id=peer(offset), device_id_type=MESH)

    def start(offset, carry):
        tell(offset).start()
        return carry

    def finish(offset, carry):
        tell(offset).wait()
        return carry

    for swap in swaps:
        swap.start()
    lax.fori_loop(1, count, start, 0)
    all_ref[me] = ids_ref[...]
    lax.fori_loop(1, count, finish, 0)
    for swap in swaps:
        swap.wait()


class Grid:
    def __init__(self, sizes):
        self.sizes = sizes
        self.slab, self.bl = lax.axis_index("slab"), lax.axis_index("bl")
        self.y, self.core = self.slab // 2, lax.rem(self.slab, 2)
        self.z, self.x = self.bl // sizes["x"], lax.rem(self.bl, sizes["x"])

    def along(self, axis, offset):
        if axis == "core":
            return (self.slab + 1 - 2 * self.core, self.bl)
        at = lax.rem(getattr(self, axis) + offset, self.sizes[axis])
        if axis == "y":
            return (at * 2 + self.core, self.bl)
        if axis == "z":
            return (self.slab, at * self.sizes["x"] + self.x)
        return (self.slab, self.z * self.sizes["x"] + at)

    def others(self):
        peers = [self.along("core", 1)]
        for axis in "yzx":
            peers += [self.along(axis, offset) for offset in range(1, self.sizes[axis])]
        return peers


def send(src, dst, sems, at, to):
    copy = pltpu.make_async_remote_copy(
        src_ref=src, dst_ref=dst, send_sem=sems.at[(0,) + at], recv_sem=sems.at[(1,) + at],
        device_id=to, device_id_type=MESH)
    copy.start()
    return copy


def reduce_kernel(
    part_ref, out_ref, r0, c0, r1a, c1a, r1b, c1b, r2a, r2b, c2, r3,
    s_own, s0, s1a, s1b, s2a, s2b, s3, *, sizes,
):
    place = Grid(sizes)
    ny, nz, nx = sizes["y"], sizes["z"], sizes["x"]
    x, y, z, core = place.x, place.y, place.z, place.core
    greet(place.others())
    owns, first = [], []
    for h in range(2):
        first.append(send(part_ref.at[:, 1 - core, :, :, h], r0.at[h], s0, (h,), place.along("core", 1)))
    for h in range(2):
        own = pltpu.make_async_copy(part_ref.at[:, core, :, :, h], c0.at[h], s_own.at[h])
        own.start()
        owns.append(own)

    def total(h):
        owns[h].wait()
        first[h].wait_recv()

        def add(at, carry):
            iy, iz, ix = at // (nz * nx), lax.rem(at // nx, nz), lax.rem(at, nx)
            c0[h, iy, iz, ix] = c0[h, iy, iz, ix] + r0[h, iy, iz, ix]
            return carry

        lax.fori_loop(0, ny * nz * nx, add, 0)

    def summed(value, got, *at):
        for o in range(got.shape[0]):
            value = value + got[(o,) + at]
        return value

    total(0)
    one_a = [send(c0.at[0, lax.rem(y + o, ny)], r1a.at[o - 1], s1a, (o - 1,), place.along("y", o))
             for o in range(1, ny)]
    total(1)
    one_b = [send(c0.at[1, :, :, lax.rem(x + o, nx)], r1b.at[o - 1], s1b, (o - 1,), place.along("x", o))
             for o in range(1, nx)]
    for copy in one_a:
        copy.wait_recv()

    def add_one_a(at, carry):
        iz, ix = at // nx, lax.rem(at, nx)
        c1a[iz, ix] = summed(c0[0, y, iz, ix], r1a, iz, ix)
        return carry

    lax.fori_loop(0, nz * nx, add_one_a, 0)
    two_a = [send(c1a.at[:, lax.rem(x + o, nx)], r2a.at[o - 1], s2a, (o - 1,), place.along("x", o))
             for o in range(1, nx)]
    for copy in one_b:
        copy.wait_recv()

    def add_one_b(at, carry):
        iy, iz = at // nz, lax.rem(at, nz)
        c1b[iy, iz] = summed(c0[1, iy, iz, x], r1b, iy, iz)
        return carry

    lax.fori_loop(0, ny * nz, add_one_b, 0)
    two_b = [send(c1b.at[lax.rem(y + o, ny)], r2b.at[o - 1], s2b, (o - 1,), place.along("y", o))
             for o in range(1, ny)]
    three = []
    for h, copies in enumerate((two_a, two_b)):
        for copy in copies:
            copy.wait_recv()

        def add_two(iz, carry):
            c2[h, iz] = summed(c1a[iz, x], r2a, iz) if h == 0 else summed(c1b[y, iz], r2b, iz)
            return carry

        lax.fori_loop(0, nz, add_two, 0)
        three.append([
            send(c2.at[h, lax.rem(z + o, nz)], r3.at[h, o - 1], s3, (h, o - 1), place.along("z", o))
            for o in range(1, nz)])
    for h in range(2):
        for copy in three[h]:
            copy.wait_recv()
        value = c2[h, z]
        for o in range(nz - 1):
            value = value + r3[h, o]
        out_ref[h] = value
    for copy in first + one_a + one_b + two_a + two_b + three[0] + three[1]:
        copy.wait_send()


def gather_kernel(mine_ref, out_ref, s_own, s_z, s_two, s_three, s_core, *, sizes):
    place = Grid(sizes)
    x, y, z, core = place.x, place.y, place.z, place.core
    greet(place.others())
    own = pltpu.make_async_copy(mine_ref, out_ref.at[y, core, z, x], s_own)
    own.start()
    along_z = [
        [send(mine_ref.at[h], out_ref.at[y, core, z, x, h], s_z, (h, o - 1), place.along("z", o))
         for o in range(1, sizes["z"])] for h in range(2)]
    own.wait()
    two = []
    for h, axis in enumerate("xy"):
        for copy in along_z[h]:
            copy.wait_recv()
        ref = out_ref.at[y, core, :, x, h]
        two.append([send(ref, ref, s_two, (h, o - 1), place.along(axis, o)) for o in range(1, sizes[axis])])
    three = []
    for h, axis in enumerate("yx"):
        for copy in two[h]:
            copy.wait_recv()
        ref = out_ref.at[y, core, :, :, 0] if h == 0 else out_ref.at[:, core, :, x, 1]
        three.append([send(ref, ref, s_three, (h, o - 1), place.along(axis, o)) for o in range(1, sizes[axis])])
    last = []
    for h in range(2):
        for copy in three[h]:
            copy.wait_recv()
        ref = out_ref.at[:, core, :, :, h]
        last.append(send(ref, ref, s_core, (h,), place.along("core", 1)))
    for copy in last:
        copy.wait_recv()
    for copy in along_z[0] + along_z[1] + two[0] + two[1] + three[0] + three[1] + last:
        copy.wait_send()


def talk(number):
    return pltpu.CompilerParams(collective_id=number, has_side_effects=True, vmem_limit_bytes=67_000_000)


def swap_and_name(image, ids, bands, groups):
    halves, wide = image.shape[:3], image.shape[3] // 2
    count = bands * groups
    return pl.pallas_call(
        functools.partial(swap_kernel, bands=bands, groups=groups),
        in_specs=[pl.BlockSpec(memory_space=pltpu.VMEM), pl.BlockSpec(memory_space=pl.ANY)],
        out_specs=[pl.BlockSpec(memory_space=pl.ANY), pl.BlockSpec(memory_space=pltpu.VMEM)],
        out_shape=[
            jax.ShapeDtypeStruct(halves + (wide,), F32),
            jax.ShapeDtypeStruct((count,) + ids.shape, jnp.int32),
        ],
        scratch_shapes=[
            pltpu.SemaphoreType.DMA(halves[:2]), pltpu.SemaphoreType.DMA(halves[:2]),
            pltpu.SemaphoreType.DMA((count,)), pltpu.SemaphoreType.DMA((count,)),
        ],
        compiler_params=talk(1),
        name="swap_columns",
    )(ids, image)


def grid_sizes(bands, groups):
    ny = bands // 2
    nx = math.gcd(groups, ny)
    return {"y": ny, "x": nx, "z": groups // nx}


def reduce_tiles(partial, bands, groups):
    sizes = grid_sizes(bands, groups)
    ny, nz, nx = sizes["y"], sizes["z"], sizes["x"]
    total, rows = partial.shape[:2]
    block = (total // (bands * groups) // 2 * rows, LANES)
    vmem = lambda *shape: pltpu.VMEM(shape + block, F32)
    sems = lambda *shape: pltpu.SemaphoreType.DMA((2,) + tuple(max(1, n) for n in shape))
    out = pl.pallas_call(
        functools.partial(reduce_kernel, sizes=sizes),
        in_specs=[pl.BlockSpec(memory_space=pl.ANY)],
        out_specs=pl.BlockSpec(memory_space=pltpu.VMEM),
        out_shape=jax.ShapeDtypeStruct((2,) + block, F32),
        scratch_shapes=[
            vmem(2, ny, nz, nx), vmem(2, ny, nz, nx),
            vmem(ny - 1, nz, nx), vmem(nz, nx),
            vmem(nx - 1, ny, nz), vmem(ny, nz),
            vmem(nx - 1, nz), vmem(ny - 1, nz), vmem(2, nz), vmem(2, nz - 1),
            pltpu.SemaphoreType.DMA((2,)), sems(2), sems(ny - 1), sems(nx - 1),
            sems(nx - 1), sems(ny - 1), sems(2, nz - 1),
        ],
        compiler_params=talk(2),
        name="reduce_tiles",
    )(partial.reshape((ny, 2, nz, nx, 2) + block))
    return out.reshape(total // (bands * groups), rows, LANES)


def gather_tiles(mine, bands, groups):
    sizes = grid_sizes(bands, groups)
    ny, nz, nx = sizes["y"], sizes["z"], sizes["x"]
    count, rows = mine.shape[:2]
    block = (count // 2 * rows, LANES)
    most = max(nx, ny) - 1
    sems = lambda *shape: pltpu.SemaphoreType.DMA((2,) + shape)
    out = pl.pallas_call(
        functools.partial(gather_kernel, sizes=sizes),
        in_specs=[pl.BlockSpec(memory_space=pltpu.VMEM)],
        out_specs=pl.BlockSpec(memory_space=pl.ANY),
        out_shape=jax.ShapeDtypeStruct((ny, 2, nz, nx, 2) + block, F32),
        scratch_shapes=[
            pltpu.SemaphoreType.DMA, sems(2, nz - 1), sems(2, most), sems(2, most), sems(2),
        ],
        compiler_params=talk(3),
        name="gather_tiles",
    )(mine.reshape((2,) + block))
    return out.reshape(bands * groups * count, rows, LANES)


def complex_table(cos, sin):
    return jnp.concatenate(
        [jnp.concatenate([cos, -sin], axis=1), jnp.concatenate([sin, cos], axis=1)], axis=0)


def per_device(model_image, vis_coords, vis_observed, tile_slot, tile_group, w_plane, vis_count):
    groups = lax.axis_size("bl")
    bands = lax.axis_size("slab")
    rows, cols = model_image.shape[1:]
    length = rows * bands
    ntile = length // SUB
    band = lax.axis_index("slab")
    core = lax.rem(band, 2)
    wide = cols // 2
    blocks = wide // LANES
    kr = 2 * rows // ntile
    swap = [(d, d ^ 1) for d in range(bands)]

    sub_count = tile_slot.shape[0]
    tile_cols = ntile // (bands * groups)
    own_tv = (band * groups + tile_group[:, 0]) * tile_cols + tile_slot // ntile
    own_tu = tile_slot % ntile
    ids = jnp.pad(jnp.stack([own_tu, own_tv]), ((0, 6), (0, LANES - sub_count)))
    shaped = model_image.reshape(2, kr // 2, ntile, cols)
    other, named = swap_and_name(shaped, ids, bands, groups)
    tu = named[:, 0, :sub_count].reshape(-1)
    tv = named[:, 1, :sub_count].reshape(-1)
    total = tu.shape[0]
    chunk = math.gcd(total, 32)
    steps = total // chunk

    inner = jnp.arange(ntile, dtype=jnp.int32)
    outer = jnp.arange(SUB, dtype=jnp.int32)
    own_cols = lax.axis_index("bl") * cols + core * wide + jnp.arange(wide, dtype=jnp.int32)
    first_row = band // 2 * (2 * rows)

    dft_c, dft_s = turn(inner[:, None] * inner[None, :], ntile)
    fwd_high, fwd_low = split(complex_table(dft_c, -dft_s))
    bwd_high, bwd_low = split(complex_table(dft_c, dft_s))
    turns = jnp.stack(turn((first_row + inner)[:, None] * outer[None, :], length), axis=2)
    turns = jnp.pad(turns.reshape(ntile, 2 * SUB), ((0, 0), (0, LANES - 2 * SUB)))
    col_c, col_s = turn(own_cols[:, None] * outer[None, :], length)
    col_c, col_s = col_c / length, col_s / length
    out_high, out_low = split(jnp.concatenate(
        [jnp.concatenate([col_c, -col_s], axis=1), jnp.concatenate([col_s, col_c], axis=1)], axis=0))
    zero = jnp.zeros_like(out_high)
    col_fwd = jnp.concatenate(
        [jnp.concatenate([out_high, out_low], axis=1), jnp.concatenate([out_high, zero], axis=1)], axis=0)
    in_high, in_low = split(jnp.concatenate(
        [jnp.concatenate([col_c.T, col_s.T], axis=1), jnp.concatenate([-col_s.T, col_c.T], axis=1)], axis=0))
    col_bwd = jnp.concatenate([in_high, in_low, in_high, in_low], axis=0)
    e_c, e_s = turn(tv[:, None] * own_cols[None, :], ntile)
    e_table = jnp.stack([e_c.reshape(total, blocks, LANES), e_s.reshape(total, blocks, LANES)], axis=2)
    e_table = e_table.reshape(total, 2 * blocks, LANES)

    whole = lambda shape: pl.BlockSpec(shape, lambda step, ids: (0,) * len(shape))
    by_step = lambda shape: pl.BlockSpec(shape, lambda step, ids: (step,) + (0,) * (len(shape) - 1))
    anywhere = pl.BlockSpec(memory_space=pl.ANY)
    params = pltpu.CompilerParams(
        dimension_semantics=("arbitrary",), vmem_limit_bytes=67_000_000)
    partial = pl.pallas_call(
        functools.partial(forward_kernel, ntile=ntile, blocks=blocks, chunk=chunk),
        grid_spec=pltpu.PrefetchScalarGridSpec(
            num_scalar_prefetch=1,
            grid=(steps,),
            in_specs=[
                anywhere, anywhere,
                whole((2 * ntile, 4 * ntile)), whole((2 * ntile, 2 * ntile)), whole((ntile, LANES)),
                whole((4 * wide, LANES)), by_step((chunk, 2 * blocks, LANES)),
            ],
            out_specs=by_step((chunk, SUB // 2, LANES)),
            scratch_shapes=[
                pltpu.VMEM((2, 2, kr, ntile, LANES), F32),
                pltpu.VMEM((SUB // 2, 4, ntile, 2 * LANES), BF16),
                pltpu.VMEM((blocks, ntile // 8, 2 * SUB * 8, LANES), F32),
                pltpu.VMEM((chunk * SUB, 4 * wide), BF16),
                pltpu.SemaphoreType.DMA((2, 2)),
            ],
        ),
        out_shape=jax.ShapeDtypeStruct((total, SUB // 2, LANES), F32),
        compiler_params=params,
        name="tiles_from_image",
    )(
        tu,
        shaped, other,
        jnp.concatenate([fwd_high, fwd_high], axis=1), fwd_low, turns, col_fwd, e_table,
    )
    mine = reduce_tiles(partial, bands, groups)
    mine = mine.reshape(sub_count, SUB // 2, 2, 2, SUB).transpose(3, 0, 2, 1, 4)
    mine = mine.reshape(2, sub_count, SUB, SUB)
    residual_vis, contrib = subgrid_pass(
        mine[0], mine[1], vis_coords, vis_observed, w_plane, vis_count)
    contrib = contrib.reshape(sub_count, 2, 2, SUB // 2, SUB).transpose(0, 3, 2, 1, 4)
    everyone = gather_tiles(contrib.reshape(sub_count, SUB // 2, LANES), bands, groups)

    image, leaving = pl.pallas_call(
        functools.partial(backward_kernel, ntile=ntile, blocks=blocks, chunk=chunk, steps=steps),
        grid_spec=pltpu.PrefetchScalarGridSpec(
            num_scalar_prefetch=1,
            grid=(steps,),
            in_specs=[
                by_step((chunk, SUB // 2, LANES)),
                whole((2 * ntile, 4 * ntile)), whole((2 * ntile, 2 * ntile)), whole((ntile, LANES)),
                whole((8 * SUB, 2 * wide)), by_step((chunk, 2 * blocks, LANES)),
            ],
            out_specs=[anywhere, anywhere],
            scratch_shapes=[
                pltpu.VMEM((2, 2, kr, ntile, LANES), F32),
                pltpu.VMEM((SUB, 2, ntile, LANES), F32),
                pltpu.VMEM((blocks, ntile // 8, 2 * SUB * 8, LANES), F32),
                pltpu.VMEM((chunk * SUB, 2 * wide), F32),
                pltpu.SemaphoreType.DMA((2, 2)),
            ],
        ),
        out_shape=[
            jax.ShapeDtypeStruct((2, kr // 2, ntile, cols), F32),
            jax.ShapeDtypeStruct((2, kr // 2, ntile, wide), F32),
        ],
        compiler_params=params,
        name="image_from_tiles",
    )(
        tu, everyone,
        jnp.concatenate([bwd_high, bwd_high], axis=1), bwd_low, turns, col_bwd, e_table,
    )
    arrived = lax.ppermute(leaving.reshape(2, rows, wide), "slab", swap)
    image = lax.dynamic_update_slice_in_dim(
        image.reshape(2, rows, cols), arrived, (1 - core) * wide, axis=2)
    return (image, residual_vis)


def solution(mesh):
    placed = (
        P(None, "slab", "bl"),
        P(("slab", "bl"), None, None),
        P(("slab", "bl"), None, None),
        P(("slab", "bl")),
        P(("slab", "bl"), None),
        P(("slab", "bl")),
        P(("slab", "bl")),
    )
    return jax.shard_map(
        per_device,
        mesh=mesh,
        in_specs=placed,
        out_specs=(P(None, "slab", "bl"), P(("slab", "bl"), None, None)),
        check_vma=False,
    )
```
